32 devices in a mesh: fsdp: 8 (over z, core), tp: 4 (over y, x).
Axes of the slice: x: 2, y: 2, z: 4, core: 2. Of those that a mesh axis runs over, the one named last changes fastest.
Arguments:
- tokens: bfloat16 [16384, 2048], P(('fsdp', 'tp')), may hold values from -6 to 6
- gain_attn: float32 [2048], replicated, may hold values from 0.25 to 1.75
- gain_mlp: float32 [2048], replicated, may hold values from 0.25 to 1.75
- w_query: bfloat16 [2048, 2048], P('fsdp', 'tp'), may hold values from -0.125 to 0.125
- w_key: bfloat16 [2048, 2048], P('fsdp', 'tp'), may hold values from -0.125 to 0.125
- w_value: bfloat16 [2048, 2048], P('fsdp', 'tp'), may hold values from -0.125 to 0.125
- w_out: bfloat16 [2048, 2048], P('fsdp', 'tp'), may hold values from -0.5 to 0.5
- w_gate: bfloat16 [2048, 8192], P('fsdp', 'tp'), may hold values from -0.125 to 0.125
- w_up: bfloat16 [2048, 8192], P('fsdp', 'tp'), may hold values from -0.125 to 0.125
- w_down: bfloat16 [2048, 8192], P('fsdp', 'tp'), may hold values from -0.0625 to 0.0625
- lengths: int32 [16], P('fsdp'), may hold values from 256 to 1024, as said below
- out_grad: bfloat16 [16384, 2048], P(('fsdp', 'tp')), may hold values from -6 to 6
Outputs:
- output: bfloat16 [16384, 2048], P(('fsdp', 'tp'))
- input_grad: bfloat16 [16384, 2048], P(('fsdp', 'tp'))
- gain_attn_grad: float32 [2048], P(('fsdp', 'tp'))
- gain_mlp_grad: float32 [2048], P(('fsdp', 'tp'))
- query_grad: float32 [2048, 2048], P('fsdp', 'tp')
- key_grad: float32 [2048, 2048], P('fsdp', 'tp')
- value_grad: float32 [2048, 2048], P('fsdp', 'tp')
- out_proj_grad: float32 [2048, 2048], P('fsdp', 'tp')
- gate_grad: float32 [2048, 8192], P('fsdp', 'tp')
- up_grad: float32 [2048, 8192], P('fsdp', 'tp')
- down_grad: float32 [2048, 8192], P('fsdp', 'tp')
The draws below stay inside these ranges and needn't reach their ends.
Inputs may be any that keep to these rules, and one draw needn't show every extreme that they name: `lengths`: valid tokens of each slot, the first ones of the slot; some slot holds exactly 1024.
All inputs are finite; a program needn't handle non-finite values.
Results may differ from the reference program's by a relative error of at most 0.02.
Values may be sent and summed in bfloat16 or wider, within the bound.
A program may use at most 448 MiB of HBM per device.

```python
import jax
import jax.numpy as jnp
from jax import lax

D = 2048
HD = 64
FF = 8192
SEQ = 1024
SLOTS = 16
TOKENS = 16384
N_FSDP = 8


def draw_lengths(key, part):
    drawn = jax.random.randint(key, (SLOTS,), SEQ // 4, SEQ + 1)
    chosen = jax.random.randint(jax.random.fold_in(key, 7), (), 0, SLOTS)
    return jnp.where(jnp.arange(SLOTS) == chosen, SEQ, drawn).astype(jnp.int32)


def block_scale(rng, extent, shards, least, top_value):
    def one(dim, parts):
        draws = jax.random.uniform(jax.random.fold_in(jax.random.fold_in(rng, 6), dim), (parts,), jnp.float32, least / len(shards), top_value / len(shards))
        return jnp.repeat(jnp.exp(draws), extent[dim] // parts).reshape((-1,) + (1,) * (len(extent) - dim - 1))

    level = one(*shards[0])
    for cut in shards[1:]:
        level = level * one(*cut)
    return level


def scatter_about(own_key, extent, spread, limit, split=(), held_as=jnp.bfloat16):
    values = jax.random.normal(own_key, extent, jnp.float32) * spread
    if len(split) > 0:
        values = block_scale(own_key, extent, split, -0.22, 0.18) * values
    return jnp.clip(values, min=-limit, max=limit).astype(held_as)


def setup_inputs(seed: int = 0) -> dict:
    seeds = jax.random.split(jax.random.key(seed), 13)
    tokens = scatter_about(seeds[0], (TOKENS, D), 1.0, 6.0, ((0, 32),))
    gain_attn = jnp.clip(1.0 + 0.15 * jax.random.normal(seeds[1], (D,), jnp.float32), 0.25, 1.75)
    gain_mlp = jnp.clip(1.0 + 0.15 * jax.random.normal(seeds[2], (D,), jnp.float32), 0.25, 1.75)
    w_query = scatter_about(seeds[3], (D, D), D ** -0.5, 0.125, ((0, 8), (1, 4)))
    w_key = scatter_about(seeds[4], (D, D), D ** -0.5, 0.125, ((0, 8), (1, 4)))
    w_value = scatter_about(seeds[5], (D, D), D ** -0.5, 0.125, ((0, 8), (1, 4)))
    w_out = scatter_about(seeds[6], (D, D), (D // 16) ** -0.5, 0.5, ((0, 8), (1, 4)))
    w_gate = scatter_about(seeds[7], (D, FF), D ** -0.5, 0.125, ((0, 8), (1, 4)))
    w_up = scatter_about(seeds[8], (D, FF), D ** -0.5, 0.125, ((0, 8), (1, 4)))
    w_down = scatter_about(seeds[9], (D, FF), FF ** -0.5, 0.0625, ((0, 8), (1, 4)))
    lengths = draw_lengths(jax.random.fold_in(seeds[12], 71), 0)
    out_grad = scatter_about(seeds[11], (TOKENS, D), 1.0, 6.0, ((0, 32),))
    return dict(tokens=tokens, gain_attn=gain_attn, gain_mlp=gain_mlp, w_query=w_query, w_key=w_key, w_value=w_value, w_out=w_out, w_gate=w_gate, w_up=w_up, w_down=w_down, lengths=lengths, out_grad=out_grad)


@jax.custom_vjp
def low(v):
    return lax.optimization_barrier(v.astype(jnp.bfloat16)).astype(jnp.float32)

@jax.custom_vjp
def low_back(v):
    return v

def low_keep(v):
    return (low(v), None)

def low_pass(kept, grad):
    return (grad,)

def back_keep(v):
    return (v, None)

def back_low(kept, grad):
    return (low(grad),)
low.defvjp(low_keep, low_pass)
low_back.defvjp(back_keep, back_low)
EPS = 1e-05
THETA = 130000.0
NEGATIVE = -1e+30
HIGH = lax.Precision.HIGHEST

def matmul(left, right):
    return jnp.dot(left, right, precision=HIGH)

def matmul_nt(left, right):
    return lax.dot_general(left, right, (((1,), (1,)), ((), ())), precision=HIGH)

def normalize(values, gain):
    return values * lax.rsqrt(lax.optimization_barrier(jnp.mean(values * values, axis=-1, keepdims=True)) + EPS) * gain

def rotary(field):
    half = HD // 2
    length = field.shape[1]
    places = jnp.arange(length, dtype=jnp.float32)[:, None]
    freqs = 1.0 / THETA ** (jnp.arange(half, dtype=jnp.float32) * 2.0 / HD)
    angle = places * freqs[None, :]
    cosine = jnp.cos(angle)[None, :, None, :]
    sine = jnp.sin(angle)[None, :, None, :]
    first = field[..., :half]
    second = field[..., half:]
    return jnp.concatenate([first * cosine - second * sine, second * cosine + first * sine], axis=-1)

def layer(tokens, gain_attn, gain_mlp, w_query, w_key, w_value, w_out, w_gate, w_up, w_down, lengths):
    count = lengths.shape[0]
    total_rows = tokens.shape[0]
    length = total_rows // count
    places = jnp.arange(length).astype(jnp.int32)
    causal = places[None, :] <= places[:, None]
    live = places[None, :] < lengths[:, None]
    allowed = causal[None, None, :, :] & live[:, None, None, :]
    valid = live.astype(jnp.float32).reshape(total_rows, 1)
    hidden_one = low(normalize(tokens, gain_attn))
    heads = w_query.shape[1] // HD

    def heads_of(weight):
        return matmul(hidden_one, weight).reshape(count, length, heads, HD)
    query = low(rotary(low_back(heads_of(w_query))))
    keys = low(rotary(low_back(heads_of(w_key))))
    values = low(low_back(heads_of(w_value)))
    scale = HD ** (-0.5)
    scores = low_back(jnp.einsum('cqhd,ckhd->chqk', query, keys, precision=HIGH) * scale)
    scores = jnp.where(allowed, scores, NEGATIVE)
    top = lax.optimization_barrier(jnp.max(scores, axis=-1, keepdims=True))
    expd = jnp.exp(scores - top)
    probs = low(expd / lax.optimization_barrier(jnp.sum(expd, axis=-1, keepdims=True)))
    attended = jnp.einsum('chqk,ckhd->cqhd', probs, values, precision=HIGH)
    mixed = low(low_back(attended.reshape(total_rows, -1)))
    middle = tokens + low_back(matmul_nt(mixed, w_out))
    hidden_two = low(normalize(middle, gain_mlp))
    gate = low_back(matmul(hidden_two, w_gate))
    upward = low_back(matmul(hidden_two, w_up))
    activated = low(jax.nn.silu(gate) * upward)
    return valid * (middle + low_back(matmul_nt(activated, w_down)))

def reference(tokens, gain_attn, gain_mlp, w_query, w_key, w_value, w_out, w_gate, w_up, w_down, lengths, out_grad):
    params = tuple((item.astype(jnp.float32) for item in (gain_attn, gain_mlp, w_query, w_key, w_value, w_out, w_gate, w_up, w_down)))
    inputs = tokens.astype(jnp.float32).reshape(N_FSDP, -1, D)
    cotangents = out_grad.astype(jnp.float32).reshape(N_FSDP, -1, D)
    group_lengths = lengths.reshape(N_FSDP, -1)

    def step(totals, item):
        group_tokens, group_grad, group_len = item

        def forward(values, *weights):
            return layer(values, *weights, group_len)
        result, pull = jax.vjp(forward, group_tokens, *params)
        grads = pull(group_grad)
        totals = tuple((total + grad for total, grad in zip(totals, grads[1:])))
        return (totals, (result, grads[0]))
    zeros = tuple((jnp.zeros_like(item) for item in params))
    totals, (results, input_grads) = lax.scan(step, zeros, (inputs, cotangents, group_lengths))
    output = results.reshape(-1, D).astype(jnp.bfloat16)
    input_grad = input_grads.reshape(-1, D).astype(jnp.bfloat16)
    return (output, input_grad, totals[0], totals[1], totals[2], totals[3], totals[4], totals[5], totals[6], totals[7], totals[8])
```

```python
import functools

import jax
import jax.numpy as jnp
from jax import lax
from jax.experimental import pallas as pl
from jax.experimental.pallas import tpu as pltpu
from jax.sharding import PartitionSpec as P

HD = 64
EPS = 1e-05
THETA = 130000.0
NEGATIVE = -1e30
QB = 256
LANES = 128
BF16 = jnp.bfloat16
F32 = jnp.float32


def matmul(left, right):
    return jnp.dot(left, right, preferred_element_type=F32)


def matmul_nt(left, right):
    return lax.dot_general(left, right, (((1,), (1,)), ((), ())), preferred_element_type=F32)


def matmul_tn(left, right):
    return lax.dot_general(left, right, (((0,), (0,)), ((), ())), preferred_element_type=F32)


def inverse_rms(values):
    return lax.rsqrt(jnp.mean(values * values, axis=-1, keepdims=True) + EPS)


def rotary_tables(length):
    half = HD // 2
    places = jnp.arange(length, dtype=F32)[:, None]
    freqs = 1.0 / THETA ** (jnp.arange(half, dtype=F32) * 2.0 / HD)
    angle = places * freqs[None, :]
    cosine, sine = jnp.cos(angle), jnp.sin(angle)
    return (
        jnp.concatenate([cosine] * 4, axis=1),
        jnp.concatenate([-sine, sine, -sine, sine], axis=1),
    )


def turn(field, cosine, sine):
    lane = lax.broadcasted_iota(jnp.int32, field.shape, 1)
    swapped = jnp.where(lane % HD < HD // 2, pltpu.roll(field, LANES - HD // 2, 1), pltpu.roll(field, HD // 2, 1))
    return field * cosine + swapped * sine


def head_lanes(rows, head):
    lane = lax.broadcasted_iota(jnp.int32, (rows, LANES), 1)
    return (lane // HD) == head


def only(values, keep):
    return jnp.where(keep, values, jnp.zeros_like(values))


def place_of(block, own, flip):
    piece, rest = divmod(block * QB, own)
    return pl.multiple_of((piece ^ flip) * own + rest, QB)


def diag_mask(block, live):
    row = lax.broadcasted_iota(jnp.int32, (QB, QB), 0)
    col = lax.broadcasted_iota(jnp.int32, (QB, QB), 1)
    return (col <= row) & (col + block * QB < live)


def attend_kernel(own, info, q_ref, k_ref, v_ref, cos_ref, sin_ref, qo, ko, vo, ao, qs, ks, vs):
    length = q_ref.shape[0]
    live, flip = info[0], info[1]
    for b in range(length // QB):
        rows = pl.ds(place_of(b, own, flip), QB)
        here = pl.ds(b * QB, QB)
        cosine, sine = cos_ref[here, :], sin_ref[here, :]
        query = (turn(q_ref[rows, :], cosine, sine) * HD ** (-0.5)).astype(BF16)
        key = turn(k_ref[rows, :], cosine, sine).astype(BF16)
        value = v_ref[rows, :].astype(BF16)
        qo[rows, :] = query
        ko[rows, :] = key
        vo[rows, :] = value
        qs[here, :] = query
        ks[here, :] = key
        vs[here, :] = value
    for b in range(length // QB):
        rows = pl.ds(place_of(b, own, flip), QB)

        @pl.when(b * QB < live)
        def _():
            allowed = diag_mask(b, live)
            outs = []
            for head in range(2):
                query = only(qs[pl.ds(b * QB, QB), :], head_lanes(QB, head))
                diag = matmul_nt(query, ks[pl.ds(b * QB, QB), :])
                diag = jnp.where(allowed, diag, NEGATIVE)
                top = jnp.max(diag, axis=1, keepdims=True)
                if b:
                    past = matmul_nt(query, ks[pl.ds(0, b * QB), :])
                    top = jnp.maximum(top, jnp.max(past, axis=1, keepdims=True))
                diag = jnp.exp(diag - top)
                total = jnp.sum(diag, axis=1, keepdims=True)
                mixed = matmul(diag.astype(BF16), vs[pl.ds(b * QB, QB), :])
                if b:
                    past = jnp.exp(past - top)
                    total = total + jnp.sum(past, axis=1, keepdims=True)
                    mixed = mixed + matmul(past.astype(BF16), vs[pl.ds(0, b * QB), :])
                outs.append(mixed / total)
            ao[rows, :] = jnp.where(head_lanes(QB, 0), outs[0], outs[1]).astype(BF16)

        @pl.when(b * QB >= live)
        def _():
            ao[rows, :] = jnp.zeros((QB, LANES), BF16)


def attend(qkv, slot, info, cosine, sine, own, length):
    width = qkv.shape[1] // 3
    pairs = width // LANES
    wide = jax.ShapeDtypeStruct((length, width), BF16)

    def column(third):
        return pl.BlockSpec((length, LANES), lambda i, s: (slot, third * pairs + i))

    whole = pl.BlockSpec((length, LANES), lambda i, s: (0, 0))
    out = pl.BlockSpec((length, LANES), lambda i, s: (0, i))
    return pl.pallas_call(
        functools.partial(attend_kernel, own),
        out_shape=[wide] * 4,
        grid_spec=pltpu.PrefetchScalarGridSpec(
            num_scalar_prefetch=1,
            grid=(pairs,),
            in_specs=[column(0), column(1), column(2), whole, whole],
            out_specs=[out] * 4,
            scratch_shapes=[pltpu.VMEM((length, LANES), BF16)] * 3,
        ),
        compiler_params=pltpu.CompilerParams(dimension_semantics=("arbitrary",)),
        cost_estimate=pl.CostEstimate(
            flops=8 * length * length * width, bytes_accessed=20 * length * width, transcendentals=0
        ),
        name="attend",
    )(info, qkv, qkv, qkv, cosine, sine)


def attend_back_kernel(own, info, q_ref, k_ref, v_ref, g_ref, cos_ref, sin_ref, out, qs, ks, vs, gs, dq, dk, dv):
    length = q_ref.shape[0]
    width = out.shape[1] // 3
    live, flip = info[0], info[1]
    pair = pl.program_id(0)
    for b in range(length // QB):
        rows = pl.ds(place_of(b, own, flip), QB)
        here = pl.ds(b * QB, QB)
        qs[here, :] = q_ref[rows, :]
        ks[here, :] = k_ref[rows, :]
        vs[here, :] = v_ref[rows, :]
        gs[here, :] = g_ref[rows, :]
    dq[...] = jnp.zeros_like(dq)
    dk[...] = jnp.zeros_like(dk)
    dv[...] = jnp.zeros_like(dv)
    for b in range(length // QB):

        @pl.when(b * QB < live)
        def _():
            here = pl.ds(b * QB, QB)
            allowed = diag_mask(b, live)
            for head in range(2):
                keep = head_lanes(QB, head)
                query = only(qs[here, :], keep)
                grad = only(gs[here, :], keep)
                diag = jnp.where(allowed, matmul_nt(query, ks[here, :]), NEGATIVE)
                top = jnp.max(diag, axis=1, keepdims=True)
                if b:
                    before = pl.ds(0, b * QB)
                    past = matmul_nt(query, ks[before, :])
                    top = jnp.maximum(top, jnp.max(past, axis=1, keepdims=True))
                diag = jnp.exp(diag - top)
                total = jnp.sum(diag, axis=1, keepdims=True)
                if b:
                    past = jnp.exp(past - top)
                    total = total + jnp.sum(past, axis=1, keepdims=True)
                scale = 1.0 / total
                diag = diag * scale
                diag_dp = matmul_nt(grad, vs[here, :])
                centre = jnp.sum(diag * diag_dp, axis=1, keepdims=True)
                if b:
                    past = past * scale
                    past_dp = matmul_nt(grad, vs[before, :])
                    centre = centre + jnp.sum(past * past_dp, axis=1, keepdims=True)
                diag_ds = (diag * (diag_dp - centre)).astype(BF16)
                dq_b = matmul(diag_ds, only(ks[here, :], keep))
                dk[here, :] += matmul_tn(diag_ds, query)
                dv[here, :] += matmul_tn(diag.astype(BF16), grad)
                if b:
                    past_ds = (past * (past_dp - centre)).astype(BF16)
                    dq_b = dq_b + matmul(past_ds, only(ks[before, :], head_lanes(b * QB, head)))
                    dk[before, :] += matmul_tn(past_ds, query)
                    dv[before, :] += matmul_tn(past.astype(BF16), grad)
                dq[here, :] += dq_b

    for b in range(length // QB):
        rows = pl.ds(place_of(b, own, flip), QB)
        here = pl.ds(b * QB, QB)
        cosine, sine = cos_ref[here, :], -sin_ref[here, :]

        def columns(third):
            return pl.ds(pl.multiple_of(third * width + pair * LANES, LANES), LANES)

        out[rows, columns(0)] = turn(dq[here, :] * HD ** (-0.5), cosine, sine).astype(BF16)
        out[rows, columns(1)] = turn(dk[here, :], cosine, sine).astype(BF16)
        out[rows, columns(2)] = dv[here, :].astype(BF16)


def attend_back(query, keys, values, grad, slot, info, cosine, sine, own, length):
    width = query.shape[1]
    pairs = width // LANES
    block = pl.BlockSpec((length, LANES), lambda i, s: (0, i))
    block_grad = pl.BlockSpec((length, LANES), lambda i, s: (slot, i))
    whole = pl.BlockSpec((length, LANES), lambda i, s: (0, 0))
    return pl.pallas_call(
        functools.partial(attend_back_kernel, own),
        out_shape=jax.ShapeDtypeStruct((length, 3 * width), BF16),
        grid_spec=pltpu.PrefetchScalarGridSpec(
            num_scalar_prefetch=1,
            grid=(pairs,),
            in_specs=[block, block, block, block_grad, whole, whole],
            out_specs=pl.BlockSpec((length, 3 * width), lambda i, s: (0, 0)),
            scratch_shapes=[pltpu.VMEM((length, LANES), BF16)] * 4 + [pltpu.VMEM((length, LANES), F32)] * 3,
        ),
        compiler_params=pltpu.CompilerParams(dimension_semantics=("arbitrary",)),
        cost_estimate=pl.CostEstimate(
            flops=20 * length * length * width, bytes_accessed=20 * length * width, transcendentals=0
        ),
        name="attend_back",
    )(info, query, keys, values, grad, cosine, sine)


def gate_up_kernel(h_ref, g_ref, u_ref, hid_ref, gate_slope, up_slope):
    gate = matmul(h_ref[...], g_ref[...])
    upward = matmul(h_ref[...], u_ref[...])
    sigma = 1.0 / (1.0 + jnp.exp(-gate))
    silu = gate * sigma
    hid_ref[...] = (silu * upward).astype(BF16)
    gate_slope[...] = (upward * sigma * (1.0 + gate * (1.0 - sigma))).astype(BF16)
    up_slope[...] = silu.astype(BF16)


def tile(extent, most):
    return min(extent, most)


def gate_up(hidden, w_gate, w_up):
    rows, depth = hidden.shape
    width = w_gate.shape[1]
    bm, bn = tile(rows, 512), tile(width, 512)
    weight = pl.BlockSpec((depth, bn), lambda j, i: (0, j))
    out = pl.BlockSpec((bm, bn), lambda j, i: (i, j))
    return pl.pallas_call(
        gate_up_kernel,
        out_shape=[jax.ShapeDtypeStruct((rows, width), BF16)] * 3,
        grid=(width // bn, rows // bm),
        in_specs=[pl.BlockSpec((bm, depth), lambda j, i: (i, 0)), weight, weight],
        out_specs=[out] * 3,
        cost_estimate=pl.CostEstimate(
            flops=4 * rows * depth * width, bytes_accessed=2 * (rows * depth + 2 * depth * width + 3 * rows * width), transcendentals=0
        ),
        name="gate_up",
    )(hidden, w_gate, w_up)


def hidden_back_kernel(g_ref, w_ref, gate_slope, up_slope, gate_out, up_out):
    grad = matmul(g_ref[...], w_ref[...])
    gate_out[...] = (grad * gate_slope[...].astype(F32)).astype(BF16)
    up_out[...] = (grad * up_slope[...].astype(F32)).astype(BF16)


def hidden_back(grad, w_down, gate_slope, up_slope):
    rows, depth = grad.shape
    width = w_down.shape[1]
    bm, bn = tile(rows, 512), tile(width, 512)
    out = pl.BlockSpec((bm, bn), lambda j, i: (i, j))
    return pl.pallas_call(
        hidden_back_kernel,
        out_shape=[jax.ShapeDtypeStruct((rows, width), BF16)] * 2,
        grid=(width // bn, rows // bm),
        in_specs=[
            pl.BlockSpec((bm, depth), lambda j, i: (i, 0)),
            pl.BlockSpec((depth, bn), lambda j, i: (0, j)),
            out,
            out,
        ],
        out_specs=[out] * 2,
        cost_estimate=pl.CostEstimate(
            flops=2 * rows * depth * width, bytes_accessed=2 * (rows * depth + depth * width + 4 * rows * width), transcendentals=0
        ),
        name="hidden_back",
    )(grad, w_down, gate_slope, up_slope)


def two_nt_kernel(a_ref, b_ref, wa_ref, wb_ref, out_ref):
    out_ref[...] = (matmul_nt(a_ref[...], wa_ref[...]) + matmul_nt(b_ref[...], wb_ref[...])).astype(BF16)


def two_nt(first, second, w_first, w_second, start, rows):
    depth = first.shape[1]
    width = w_first.shape[0]
    bm, bn = tile(rows, 512), tile(width, 512)
    left = pl.BlockSpec((bm, depth), lambda j, i: (start // bm + i, 0))
    weight = pl.BlockSpec((bn, depth), lambda j, i: (j, 0))
    return pl.pallas_call(
        two_nt_kernel,
        out_shape=jax.ShapeDtypeStruct((rows, width), BF16),
        grid=(width // bn, rows // bm),
        in_specs=[left, left, weight, weight],
        out_specs=pl.BlockSpec((bm, bn), lambda j, i: (i, j)),
        cost_estimate=pl.CostEstimate(
            flops=4 * rows * depth * width, bytes_accessed=2 * (2 * rows * depth + 2 * depth * width + rows * width), transcendentals=0
        ),
        name="two_nt",
    )(first, second, w_first, w_second)


def hop(value, bit, size):
    return lax.ppermute(value, "tp", [(i, i ^ bit) for i in range(size)])


def bit_orders(size):
    bits = []
    bit = 1
    while bit < size:
        bits.append(bit)
        bit *= 2
    return (bits, bits[::-1])


def gather_tp(halves, size):
    got = []
    for half, order in zip(halves, bit_orders(size)):
        have = {0: half}
        for bit in order:
            for r in sorted(have):
                have[r ^ bit] = hop(have[r], bit, size)
        got.append(have)
    return jnp.concatenate([got[h][r] for r in range(size) for h in range(2)], axis=0)


def scatter_tp(piece, size):
    out = []
    parts = [piece(r) for r in range(size)]
    own = parts[0].shape[0]
    for h, order in enumerate(bit_orders(size)):
        have = {r: parts[r][h * (own // 2) : (h + 1) * (own // 2)] for r in range(size)}
        for step, bit in enumerate(order[::-1]):
            last = step == len(order) - 1
            for r in sorted(have, reverse=True):
                if r & bit:
                    came = hop(have.pop(r), bit, size).astype(F32)
                    total = have[r ^ bit].astype(F32) + came
                    have[r ^ bit] = total if last else total.astype(BF16)
        out.append(have[0].astype(F32))
    return out


def split_halves(rows):
    middle = rows.shape[0] // 2
    return [rows[:middle], rows[middle:]]


def per_device(
    tokens, gain_attn, gain_mlp, w_query, w_key, w_value, w_out, w_gate, w_up, w_down, lengths, out_grad
):
    size = lax.axis_size("tp")
    me = lax.axis_index("tp")
    own = tokens.shape[0]
    count = lengths.shape[0]
    group = own * size
    length = group // count
    per_slot = length // own
    my_slot = me // per_slot
    flip = me % per_slot
    head_width = w_query.shape[1]

    def along_fsdp(weight):
        return lax.all_gather(weight, "fsdp", axis=0, tiled=True)

    qkv_full = along_fsdp(jnp.concatenate([w_query, w_key, w_value], axis=1))
    out_full = along_fsdp(w_out)
    gate_full = along_fsdp(w_gate)
    up_full = along_fsdp(w_up)
    down_full = along_fsdp(w_down)

    own_length = lax.dynamic_index_in_dim(lengths, my_slot, keepdims=False)
    places = flip * own + jnp.arange(own, dtype=jnp.int32)
    valid = split_halves((places < own_length).astype(F32)[:, None])
    infos = [
        jnp.stack([lax.dynamic_index_in_dim(lengths, my_slot ^ s, keepdims=False), flip]).astype(jnp.int32)
        for s in range(count)
    ]
    cosine, sine = rotary_tables(length)
    x = [half.astype(F32) for half in split_halves(tokens)]
    scale_one = [inverse_rms(v) for v in x]
    normed_one = [v * s for v, s in zip(x, scale_one)]
    h1 = gather_tp([(n * gain_attn).astype(BF16) for n in normed_one], size)
    grad_rows = [m * g.astype(F32) for m, g in zip(valid, split_halves(out_grad))]
    dm = gather_tp([g.astype(BF16) for g in grad_rows], size)

    qkv = matmul(h1, qkv_full)
    saved = {}
    partial = {}
    for s in reversed(range(count)):
        saved[s] = attend(qkv, s, infos[s], cosine, sine, own, length)
        partial[s] = matmul_nt(saved[s][3], out_full).astype(BF16)

    def attn_piece(r):
        s, inside = divmod(r, per_slot)
        return partial[s][inside * own : (inside + 1) * own]

    attn_out = scatter_tp(attn_piece, size)
    middle = [v + a for v, a in zip(x, attn_out)]
    scale_two = [inverse_rms(v) for v in middle]
    normed_two = [v * s for v, s in zip(middle, scale_two)]
    h2 = gather_tp([(n * gain_mlp).astype(BF16) for n in normed_two], size)

    hid, gate_slope, up_slope = gate_up(h2, gate_full, up_full)
    down_term = matmul_tn(dm, hid).astype(BF16)
    grad_gate, grad_up = hidden_back(dm, down_full, gate_slope, up_slope)
    gate_term = matmul_tn(h2, grad_gate).astype(BF16)
    up_term = matmul_tn(h2, grad_up).astype(BF16)
    half_group = group // 2
    two = [two_nt(grad_gate, grad_up, gate_full, up_full, half_group * i, half_group) for i in range(2)]

    def two_piece(r):
        i, inside = divmod(r, size // 2)
        return two[i][inside * own : (inside + 1) * own]

    grad_two = scatter_tp(two_piece, size)
    mlp = matmul_nt(hid, down_full).astype(BF16)
    mlp_out = scatter_tp(lambda r: mlp[r * own : (r + 1) * own], size)
    output = jnp.concatenate(
        [(m * (v + o)).astype(BF16) for m, v, o in zip(valid, middle, mlp_out)], axis=0
    )
    gain_mlp_term = sum(jnp.sum(g * n, axis=0) for g, n in zip(grad_two, normed_two))
    inner_two = [g * gain_mlp for g in grad_two]
    grad_middle = [
        g + s * (i - n * jnp.mean(i * n, axis=-1, keepdims=True))
        for g, s, i, n in zip(grad_rows, scale_two, inner_two, normed_two)
    ]
    grad_attn = gather_tp([g.astype(BF16) for g in grad_middle], size)

    mixed = jnp.concatenate([saved[s][3] for s in range(count)], axis=0)
    out_term = matmul_tn(grad_attn, mixed).astype(BF16)
    grad_mixed = matmul(grad_attn, out_full).astype(BF16)
    grad_qkv = {}
    partial_one = {}
    for s in reversed(range(count)):
        query, keys, values, _ = saved[s]
        grad_qkv[s] = attend_back(query, keys, values, grad_mixed, s, infos[s], cosine, sine, own, length)
        partial_one[s] = matmul_nt(grad_qkv[s], qkv_full).astype(BF16)
    qkv_term = matmul_tn(h1, jnp.concatenate([grad_qkv[s] for s in range(count)], axis=0)).astype(BF16)

    def one_piece(r):
        s, inside = divmod(r, per_slot)
        return partial_one[s][inside * own : (inside + 1) * own]

    grad_one = scatter_tp(one_piece, size)
    gain_attn_term = sum(jnp.sum(g * n, axis=0) for g, n in zip(grad_one, normed_one))
    inner_one = [g * gain_attn for g in grad_one]
    input_grad = jnp.concatenate(
        [
            (m + s * (i - n * jnp.mean(i * n, axis=-1, keepdims=True))).astype(BF16)
            for m, s, i, n in zip(grad_middle, scale_one, inner_one, normed_one)
        ],
        axis=0,
    )

    def back_fsdp(term):
        return lax.psum_scatter(term, "fsdp", scatter_dimension=0, tiled=True).astype(F32)

    down_grad = back_fsdp(down_term)
    gate_grad = back_fsdp(gate_term)
    up_grad = back_fsdp(up_term)
    out_proj_grad = back_fsdp(out_term)
    qkv_grad = back_fsdp(qkv_term)
    gains = [
        lax.psum_scatter(term, ("fsdp", "tp"), scatter_dimension=0, tiled=True)
        for term in (gain_attn_term, gain_mlp_term)
    ]
    return (
        output,
        input_grad,
        gains[0],
        gains[1],
        qkv_grad[:, :head_width],
        qkv_grad[:, head_width : 2 * head_width],
        qkv_grad[:, 2 * head_width :],
        out_proj_grad,
        gate_grad,
        up_grad,
        down_grad,
    )


def solution(mesh):
    rows = P(("fsdp", "tp"), None)
    weight = P("fsdp", "tp")
    vector = P(("fsdp", "tp"))
    return jax.shard_map(
        per_device,
        mesh=mesh,
        in_specs=(rows, P(), P()) + (weight,) * 7 + (P("fsdp"), rows),
        out_specs=(rows, rows, vector, vector) + (weight,) * 7,
        check_vma=False,
    )
```

```python
import functools

import jax
import jax.numpy as jnp
from jax import lax
from jax.experimental import pallas as pl
from jax.experimental.pallas import tpu as pltpu
from jax.sharding import PartitionSpec as P


HD = 64
EPS = 1e-05
THETA = 130000.0
NEGATIVE = -1e30
QB = 256
LANES = 128
BF16 = jnp.bfloat16
F32 = jnp.float32


def matmul(left, right):
    return jnp.dot(left, right, preferred_element_type=F32)


def matmul_nt(left, right):
    return lax.dot_general(left, right, (((1,), (1,)), ((), ())), preferred_element_type=F32)


def matmul_tn(left, right):
    return lax.dot_general(left, right, (((0,), (0,)), ((), ())), preferred_element_type=F32)


def inverse_rms(values):
    return lax.rsqrt(jnp.mean(values * values, axis=-1, keepdims=True) + EPS)


def rotary_tables(length):
    half = HD // 2
    places = jnp.arange(length, dtype=F32)[:, None]
    freqs = 1.0 / THETA ** (jnp.arange(half, dtype=F32) * 2.0 / HD)
    angle = places * freqs[None, :]
    cosine, sine = jnp.cos(angle), jnp.sin(angle)
    return (
        jnp.concatenate([cosine] * 4, axis=1),
        jnp.concatenate([-sine, sine, -sine, sine], axis=1),
    )


def turn(field, cosine, sine):
    lane = lax.broadcasted_iota(jnp.int32, field.shape, 1)
    swapped = jnp.where(lane % HD < HD // 2, pltpu.roll(field, LANES - HD // 2, 1), pltpu.roll(field, HD // 2, 1))
    return field * cosine + swapped * sine


def head_lanes(rows, head):
    lane = lax.broadcasted_iota(jnp.int32, (rows, LANES), 1)
    return (lane // HD) == head


def only(values, keep):
    return jnp.where(keep, values, jnp.zeros_like(values))


def place_of(block, own, flip):
    piece, rest = divmod(block * QB, own)
    return pl.multiple_of((piece ^ flip) * own + rest, QB)


def diag_mask(block, live):
    row = lax.broadcasted_iota(jnp.int32, (QB, QB), 0)
    col = lax.broadcasted_iota(jnp.int32, (QB, QB), 1)
    return (col <= row) & (col + block * QB < live)


def attend_kernel(own, info, q_ref, k_ref, v_ref, cos_ref, sin_ref, qo, ko, vo, ao, qs, ks, vs):
    length = q_ref.shape[0]
    live, flip = info[0], info[1]
    for b in range(length // QB):
        rows = pl.ds(place_of(b, own, flip), QB)
        here = pl.ds(b * QB, QB)
        cosine, sine = cos_ref[here, :], sin_ref[here, :]
        query = (turn(q_ref[rows, :], cosine, sine) * HD ** (-0.5)).astype(BF16)
        key = turn(k_ref[rows, :], cosine, sine).astype(BF16)
        value = v_ref[rows, :].astype(BF16)
        qo[rows, :] = query
        ko[rows, :] = key
        vo[rows, :] = value
        qs[here, :] = query
        ks[here, :] = key
        vs[here, :] = value
    for b in range(length // QB):
        rows = pl.ds(place_of(b, own, flip), QB)

        @pl.when(b * QB < live)
        def _():
            allowed = diag_mask(b, live)
            outs = []
            for head in range(2):
                query = only(qs[pl.ds(b * QB, QB), :], head_lanes(QB, head))
                diag = matmul_nt(query, ks[pl.ds(b * QB, QB), :])
                diag = jnp.where(allowed, diag, NEGATIVE)
                top = jnp.max(diag, axis=1, keepdims=True)
                if b:
                    past = matmul_nt(query, ks[pl.ds(0, b * QB), :])
                    top = jnp.maximum(top, jnp.max(past, axis=1, keepdims=True))
                diag = jnp.exp(diag - top)
                total = jnp.sum(diag, axis=1, keepdims=True)
                mixed = matmul(diag.astype(BF16), vs[pl.ds(b * QB, QB), :])
                if b:
                    past = jnp.exp(past - top)
                    total = total + jnp.sum(past, axis=1, keepdims=True)
                    mixed = mixed + matmul(past.astype(BF16), vs[pl.ds(0, b * QB), :])
                outs.append(mixed / total)
            ao[rows, :] = jnp.where(head_lanes(QB, 0), outs[0], outs[1]).astype(BF16)

        @pl.when(b * QB >= live)
        def _():
            ao[rows, :] = jnp.zeros((QB, LANES), BF16)


def attend(qkv, slot, info, cosine, sine, own, length):
    width = qkv.shape[1] // 3
    pairs = width // LANES
    wide = jax.ShapeDtypeStruct((length, width), BF16)

    def column(third):
        return pl.BlockSpec((length, LANES), lambda i, s: (slot, third * pairs + i))

    whole = pl.BlockSpec((length, LANES), lambda i, s: (0, 0))
    out = pl.BlockSpec((length, LANES), lambda i, s: (0, i))
    return pl.pallas_call(
        functools.partial(attend_kernel, own),
        out_shape=[wide] * 4,
        grid_spec=pltpu.PrefetchScalarGridSpec(
            num_scalar_prefetch=1,
            grid=(pairs,),
            in_specs=[column(0), column(1), column(2), whole, whole],
            out_specs=[out] * 4,
            scratch_shapes=[pltpu.VMEM((length, LANES), BF16)] * 3,
        ),
        compiler_params=pltpu.CompilerParams(dimension_semantics=("arbitrary",)),
        cost_estimate=pl.CostEstimate(
            flops=8 * length * length * width, bytes_accessed=20 * length * width, transcendentals=0
        ),
        name="attend",
    )(info, qkv, qkv, qkv, cosine, sine)


def attend_back_kernel(own, info, q_ref, k_ref, v_ref, g_ref, cos_ref, sin_ref, out, qs, ks, vs, gs, dq, dk, dv):
    length = q_ref.shape[0]
    width = out.shape[1] // 3
    live, flip = info[0], info[1]
    pair = pl.program_id(0)
    for b in range(length // QB):
        rows = pl.ds(place_of(b, own, flip), QB)
        here = pl.ds(b * QB, QB)
        qs[here, :] = q_ref[rows, :]
        ks[here, :] = k_ref[rows, :]
        vs[here, :] = v_ref[rows, :]
        gs[here, :] = g_ref[rows, :]
    dq[...] = jnp.zeros_like(dq)
    dk[...] = jnp.zeros_like(dk)
    dv[...] = jnp.zeros_like(dv)
    for b in range(length // QB):

        @pl.when(b * QB < live)
        def _():
            here = pl.ds(b * QB, QB)
            allowed = diag_mask(b, live)
            for head in range(2):
                keep = head_lanes(QB, head)
                query = only(qs[here, :], keep)
                grad = only(gs[here, :], keep)
                diag = jnp.where(allowed, matmul_nt(query, ks[here, :]), NEGATIVE)
                top = jnp.max(diag, axis=1, keepdims=True)
                if b:
                    before = pl.ds(0, b * QB)
                    past = matmul_nt(query, ks[before, :])
                    top = jnp.maximum(top, jnp.max(past, axis=1, keepdims=True))
                diag = jnp.exp(diag - top)
                total = jnp.sum(diag, axis=1, keepdims=True)
                if b:
                    past = jnp.exp(past - top)
                    total = total + jnp.sum(past, axis=1, keepdims=True)
                scale = 1.0 / total
                diag = diag * scale
                diag_dp = matmul_nt(grad, vs[here, :])
                centre = jnp.sum(diag * diag_dp, axis=1, keepdims=True)
                if b:
                    past = past * scale
                    past_dp = matmul_nt(grad, vs[before, :])
                    centre = centre + jnp.sum(past * past_dp, axis=1, keepdims=True)
                diag_ds = (diag * (diag_dp - centre)).astype(BF16)
                dq_b = matmul(diag_ds, only(ks[here, :], keep))
                dk[here, :] += matmul_tn(diag_ds, query)
                dv[here, :] += matmul_tn(diag.astype(BF16), grad)
                if b:
                    past_ds = (past * (past_dp - centre)).astype(BF16)
                    dq_b = dq_b + matmul(past_ds, only(ks[before, :], head_lanes(b * QB, head)))
                    dk[before, :] += matmul_tn(past_ds, query)
                    dv[before, :] += matmul_tn(past.astype(BF16), grad)
                dq[here, :] += dq_b

    for b in range(length // QB):
        rows = pl.ds(place_of(b, own, flip), QB)
        here = pl.ds(b * QB, QB)
        cosine, sine = cos_ref[here, :], -sin_ref[here, :]

        def columns(third):
            return pl.ds(pl.multiple_of(third * width + pair * LANES, LANES), LANES)

        out[rows, columns(0)] = turn(dq[here, :] * HD ** (-0.5), cosine, sine).astype(BF16)
        out[rows, columns(1)] = turn(dk[here, :], cosine, sine).astype(BF16)
        out[rows, columns(2)] = dv[here, :].astype(BF16)


def attend_back(query, keys, values, grad, slot, info, cosine, sine, own, length):
    width = query.shape[1]
    pairs = width // LANES
    block = pl.BlockSpec((length, LANES), lambda i, s: (0, i))
    block_grad = pl.BlockSpec((length, LANES), lambda i, s: (slot, i))
    whole = pl.BlockSpec((length, LANES), lambda i, s: (0, 0))
    return pl.pallas_call(
        functools.partial(attend_back_kernel, own),
        out_shape=jax.ShapeDtypeStruct((length, 3 * width), BF16),
        grid_spec=pltpu.PrefetchScalarGridSpec(
            num_scalar_prefetch=1,
            grid=(pairs,),
            in_specs=[block, block, block, block_grad, whole, whole],
            out_specs=pl.BlockSpec((length, 3 * width), lambda i, s: (0, 0)),
            scratch_shapes=[pltpu.VMEM((length, LANES), BF16)] * 4 + [pltpu.VMEM((length, LANES), F32)] * 3,
        ),
        compiler_params=pltpu.CompilerParams(dimension_semantics=("arbitrary",)),
        cost_estimate=pl.CostEstimate(
            flops=20 * length * length * width, bytes_accessed=20 * length * width, transcendentals=0
        ),
        name="attend_back",
    )(info, query, keys, values, grad, cosine, sine)


def gate_up_kernel(h_ref, g_ref, u_ref, hid_ref, gate_slope, up_slope):
    gate = matmul(h_ref[...], g_ref[...])
    upward = matmul(h_ref[...], u_ref[...])
    sigma = 1.0 / (1.0 + jnp.exp(-gate))
    silu = gate * sigma
    hid_ref[...] = (silu * upward).astype(BF16)
    gate_slope[...] = (upward * sigma * (1.0 + gate * (1.0 - sigma))).astype(BF16)
    up_slope[...] = silu.astype(BF16)


def tile(extent, most):
    return min(extent, most)


def gate_up(hidden, w_gate, w_up):
    rows, depth = hidden.shape
    width = w_gate.shape[1]
    bm, bn = tile(rows, 512), tile(width, 512)
    weight = pl.BlockSpec((depth, bn), lambda j, i: (0, j))
    out = pl.BlockSpec((bm, bn), lambda j, i: (i, j))
    return pl.pallas_call(
        gate_up_kernel,
        out_shape=[jax.ShapeDtypeStruct((rows, width), BF16)] * 3,
        grid=(width // bn, rows // bm),
        in_specs=[pl.BlockSpec((bm, depth), lambda j, i: (i, 0)), weight, weight],
        out_specs=[out] * 3,
        cost_estimate=pl.CostEstimate(
            flops=4 * rows * depth * width, bytes_accessed=2 * (rows * depth + 2 * depth * width + 3 * rows * width), transcendentals=0
        ),
        name="gate_up",
    )(hidden, w_gate, w_up)


def hidden_back_kernel(g_ref, w_ref, gate_slope, up_slope, gate_out, up_out):
    grad = matmul(g_ref[...], w_ref[...])
    gate_out[...] = (grad * gate_slope[...].astype(F32)).astype(BF16)
    up_out[...] = (grad * up_slope[...].astype(F32)).astype(BF16)


def hidden_back(grad, w_down, gate_slope, up_slope):
    rows, depth = grad.shape
    width = w_down.shape[1]
    bm, bn = tile(rows, 512), tile(width, 512)
    out = pl.BlockSpec((bm, bn), lambda j, i: (i, j))
    return pl.pallas_call(
        hidden_back_kernel,
        out_shape=[jax.ShapeDtypeStruct((rows, width), BF16)] * 2,
        grid=(width // bn, rows // bm),
        in_specs=[
            pl.BlockSpec((bm, depth), lambda j, i: (i, 0)),
            pl.BlockSpec((depth, bn), lambda j, i: (0, j)),
            out,
            out,
        ],
        out_specs=[out] * 2,
        cost_estimate=pl.CostEstimate(
            flops=2 * rows * depth * width, bytes_accessed=2 * (rows * depth + depth * width + 4 * rows * width), transcendentals=0
        ),
        name="hidden_back",
    )(grad, w_down, gate_slope, up_slope)


def two_nt_kernel(a_ref, b_ref, wa_ref, wb_ref, out_ref):
    out_ref[...] = (matmul_nt(a_ref[...], wa_ref[...]) + matmul_nt(b_ref[...], wb_ref[...])).astype(BF16)


def two_nt(first, second, w_first, w_second, start, rows):
    depth = first.shape[1]
    width = w_first.shape[0]
    bm, bn = tile(rows, 512), tile(width, 512)
    left = pl.BlockSpec((bm, depth), lambda j, i: (start // bm + i, 0))
    weight = pl.BlockSpec((bn, depth), lambda j, i: (j, 0))
    return pl.pallas_call(
        two_nt_kernel,
        out_shape=jax.ShapeDtypeStruct((rows, width), BF16),
        grid=(width // bn, rows // bm),
        in_specs=[left, left, weight, weight],
        out_specs=pl.BlockSpec((bm, bn), lambda j, i: (i, j)),
        cost_estimate=pl.CostEstimate(
            flops=4 * rows * depth * width, bytes_accessed=2 * (2 * rows * depth + 2 * depth * width + rows * width), transcendentals=0
        ),
        name="two_nt",
    )(first, second, w_first, w_second)


def hop(value, bit, size):
    return lax.ppermute(value, "tp", [(i, i ^ bit) for i in range(size)])


def bit_orders(size):
    bits = []
    bit = 1
    while bit < size:
        bits.append(bit)
        bit *= 2
    return (bits, bits[::-1])


def gather_tp(halves, size):
    got = []
    for half, order in zip(halves, bit_orders(size)):
        have = {0: half}
        for bit in order:
            for r in sorted(have):
                have[r ^ bit] = hop(have[r], bit, size)
        got.append(have)
    return jnp.concatenate([got[h][r] for r in range(size) for h in range(2)], axis=0)


def scatter_tp(piece, size):
    out = []
    parts = [piece(r) for r in range(size)]
    own = parts[0].shape[0]
    for h, order in enumerate(bit_orders(size)):
        have = {r: parts[r][h * (own // 2) : (h + 1) * (own // 2)] for r in range(size)}
        for step, bit in enumerate(order[::-1]):
            last = step == len(order) - 1
            for r in sorted(have, reverse=True):
                if r & bit:
                    came = hop(have.pop(r), bit, size).astype(F32)
                    total = have[r ^ bit].astype(F32) + came
                    have[r ^ bit] = total if last else total.astype(BF16)
        out.append(have[0].astype(F32))
    return out


def after(value, *others):
    return lax.optimization_barrier((value,) + others)[0]


def scatter_vectors(values):
    axes = ("fsdp", "tp")
    devices = lax.axis_size("fsdp") * lax.axis_size("tp")
    index = lax.axis_index("fsdp") * lax.axis_size("tp") + lax.axis_index("tp")
    bit = devices // 2
    while bit:
        pair = values.reshape(values.shape[0], 2, values.shape[1] // 2)
        mine = (index // bit) % 2
        kept = lax.dynamic_index_in_dim(pair, mine, axis=1, keepdims=False)
        sent = lax.dynamic_index_in_dim(pair, 1 - mine, axis=1, keepdims=False)
        values = kept + lax.ppermute(sent, axes, [(i, i ^ bit) for i in range(devices)])
        bit //= 2
    return values


def split_halves(rows):
    middle = rows.shape[0] // 2
    return [rows[:middle], rows[middle:]]


def per_device(
    tokens, gain_attn, gain_mlp, w_query, w_key, w_value, w_out, w_gate, w_up, w_down, lengths, out_grad
):
    size = lax.axis_size("tp")
    me = lax.axis_index("tp")
    own = tokens.shape[0]
    count = lengths.shape[0]
    group = own * size
    length = group // count
    per_slot = length // own
    my_slot = me // per_slot
    flip = me % per_slot
    head_width = w_query.shape[1]

    def along_fsdp(weight):
        return lax.all_gather(weight, "fsdp", axis=0, tiled=True)

    qkv_full = along_fsdp(jnp.concatenate([w_query, w_key, w_value], axis=1))
    out_full = along_fsdp(w_out)
    gate_full = along_fsdp(w_gate)
    up_full = along_fsdp(w_up)
    down_full = along_fsdp(w_down)

    own_length = lax.dynamic_index_in_dim(lengths, my_slot, keepdims=False)
    places = flip * own + jnp.arange(own, dtype=jnp.int32)
    valid = split_halves((places < own_length).astype(F32)[:, None])
    infos = [
        jnp.stack([lax.dynamic_index_in_dim(lengths, my_slot ^ s, keepdims=False), flip]).astype(jnp.int32)
        for s in range(count)
    ]
    cosine, sine = rotary_tables(length)
    x = [half.astype(F32) for half in split_halves(tokens)]
    scale_one = [inverse_rms(v) for v in x]
    normed_one = [v * s for v, s in zip(x, scale_one)]
    h1 = gather_tp([(n * gain_attn).astype(BF16) for n in normed_one], size)
    grad_rows = [m * g.astype(F32) for m, g in zip(valid, split_halves(out_grad))]
    dm = gather_tp([after(g.astype(BF16), h1) for g in grad_rows], size)

    qkv = matmul(h1, qkv_full)
    saved = {}
    partial = {}
    for s in reversed(range(count)):
        saved[s] = attend(qkv, s, infos[s], cosine, sine, own, length)
        partial[s] = matmul_nt(saved[s][3], out_full).astype(BF16)

    def attn_piece(r):
        s, inside = divmod(r, per_slot)
        return partial[s][inside * own : (inside + 1) * own]

    attn_out = scatter_tp(attn_piece, size)
    middle = [v + a for v, a in zip(x, attn_out)]
    scale_two = [inverse_rms(v) for v in middle]
    normed_two = [v * s for v, s in zip(middle, scale_two)]
    h2 = gather_tp([(n * gain_mlp).astype(BF16) for n in normed_two], size)

    hid, gate_slope, up_slope = gate_up(h2, gate_full, up_full)
    down_term = matmul_tn(dm, hid).astype(BF16)
    grad_gate, grad_up = hidden_back(dm, down_full, after(gate_slope, down_term), up_slope)
    half_group = group // 2
    two = {}
    two[1] = two_nt(grad_gate, grad_up, gate_full, up_full, half_group, half_group)
    two[0] = two_nt(after(grad_gate, two[1]), grad_up, gate_full, up_full, 0, half_group)
    gate_term = matmul_tn(h2, after(grad_gate, two[0])).astype(BF16)
    up_term = matmul_tn(h2, after(grad_up, gate_term)).astype(BF16)
    mlp = matmul_nt(after(hid, up_term), down_full).astype(BF16)

    def two_piece(r):
        i, inside = divmod(r, size // 2)
        return two[i][inside * own : (inside + 1) * own]

    grad_two = scatter_tp(two_piece, size)
    gain_mlp_term = sum(jnp.sum(g * n, axis=0) for g, n in zip(grad_two, normed_two))
    inner_two = [g * gain_mlp for g in grad_two]
    grad_middle = [
        g + s * (i - n * jnp.mean(i * n, axis=-1, keepdims=True))
        for g, s, i, n in zip(grad_rows, scale_two, inner_two, normed_two)
    ]
    grad_attn = gather_tp([after(g.astype(BF16), gate_term, up_term) for g in grad_middle], size)
    mlp, grad_attn = lax.optimization_barrier((mlp, grad_attn))
    mlp_out = scatter_tp(lambda r: mlp[r * own : (r + 1) * own], size)
    output = jnp.concatenate(
        [(m * (v + o)).astype(BF16) for m, v, o in zip(valid, middle, mlp_out)], axis=0
    )

    grad_mixed = matmul(grad_attn, out_full).astype(BF16)
    grad_qkv = {}
    partial_one = {}
    last = None
    for s in reversed(range(count)):
        query, keys, values, _ = saved[s]
        if last is not None:
            query = after(query, last)
        grad_qkv[s] = attend_back(query, keys, values, grad_mixed, s, infos[s], cosine, sine, own, length)
        if s:
            last = partial_one[s] = matmul_nt(grad_qkv[s], qkv_full).astype(BF16)
        if s == count - 1:
            mixed = after(jnp.concatenate([saved[i][3] for i in range(count)], axis=0), last)
            last = out_term = matmul_tn(grad_attn, mixed).astype(BF16)
    qkv_term = matmul_tn(h1, jnp.concatenate([grad_qkv[s] for s in range(count)], axis=0)).astype(BF16)
    partial_one[0] = matmul_nt(after(grad_qkv[0], qkv_term), qkv_full).astype(BF16)

    def one_piece(r):
        s, inside = divmod(r, per_slot)
        return partial_one[s][inside * own : (inside + 1) * own]

    grad_one = scatter_tp(one_piece, size)
    gain_attn_term = sum(jnp.sum(g * n, axis=0) for g, n in zip(grad_one, normed_one))
    inner_one = [g * gain_attn for g in grad_one]
    input_grad = jnp.concatenate(
        [
            (m + s * (i - n * jnp.mean(i * n, axis=-1, keepdims=True))).astype(BF16)
            for m, s, i, n in zip(grad_middle, scale_one, inner_one, normed_one)
        ],
        axis=0,
    )

    def back_fsdp(term):
        return lax.psum_scatter(term, "fsdp", scatter_dimension=0, tiled=True).astype(F32)

    down_grad = back_fsdp(down_term)
    gate_grad = back_fsdp(gate_term)
    up_grad = back_fsdp(up_term)
    out_proj_grad = back_fsdp(out_term)
    qkv_grad = back_fsdp(qkv_term)
    gains = scatter_vectors(jnp.stack([gain_attn_term, gain_mlp_term]))
    return (
        output,
        input_grad,
        gains[0],
        gains[1],
        qkv_grad[:, :head_width],
        qkv_grad[:, head_width : 2 * head_width],
        qkv_grad[:, 2 * head_width :],
        out_proj_grad,
        gate_grad,
        up_grad,
        down_grad,
    )


def solution(mesh):
    rows = P(("fsdp", "tp"), None)
    weight = P("fsdp", "tp")
    vector = P(("fsdp", "tp"))
    return jax.shard_map(
        per_device,
        mesh=mesh,
        in_specs=(rows, P(), P()) + (weight,) * 7 + (P("fsdp"), rows),
        out_specs=(rows, rows, vector, vector) + (weight,) * 7,
        check_vma=False,
    )
```

```python
import functools

import jax
import jax.numpy as jnp
from jax import lax
from jax.experimental import pallas as pl
from jax.experimental.pallas import tpu as pltpu
from jax.sharding import PartitionSpec as P


HD = 64
EPS = 1e-05
THETA = 130000.0
NEGATIVE = -1e30
QB = 256
LANES = 128
BF16 = jnp.bfloat16
F32 = jnp.float32


def matmul(left, right):
    return jnp.dot(left, right, preferred_element_type=F32)


def matmul_nt(left, right):
    return lax.dot_general(left, right, (((1,), (1,)), ((), ())), preferred_element_type=F32)


def matmul_tn(left, right):
    return lax.dot_general(left, right, (((0,), (0,)), ((), ())), preferred_element_type=F32)


def inverse_rms(values):
    return lax.rsqrt(jnp.mean(values * values, axis=-1, keepdims=True) + EPS)


def rotary_tables(length):
    half = HD // 2
    places = jnp.arange(length, dtype=F32)[:, None]
    freqs = 1.0 / THETA ** (jnp.arange(half, dtype=F32) * 2.0 / HD)
    angle = places * freqs[None, :]
    cosine, sine = jnp.cos(angle), jnp.sin(angle)
    return (
        jnp.concatenate([cosine] * 4, axis=1),
        jnp.concatenate([-sine, sine, -sine, sine], axis=1),
    )


def turn(field, cosine, sine):
    lane = lax.broadcasted_iota(jnp.int32, (1, LANES), 1)
    swapped = jnp.where((lane & (HD - 1)) < HD // 2, pltpu.roll(field, LANES - HD // 2, 1), pltpu.roll(field, HD // 2, 1))
    return field * cosine + swapped * sine


def head_lanes(head):
    lane = lax.broadcasted_iota(jnp.int32, (1, LANES), 1)
    return lane >= HD if head else lane < HD


def only(values, keep):
    return jnp.where(keep, values, jnp.zeros_like(values))


def place_of(block, own, flip):
    piece, rest = divmod(block * QB, own)
    return pl.multiple_of((piece ^ flip) * own + rest, QB)


def diag_mask(block, live):
    key = lax.broadcasted_iota(jnp.int32, (QB, QB), 0)
    query = lax.broadcasted_iota(jnp.int32, (QB, QB), 1)
    return (key <= query) & (key + block * QB < live)


def attend_kernel(own, info, q_ref, k_ref, v_ref, cos_ref, sin_ref, qo, ko, vo, ao, lo, qs, ks, vt):
    length = q_ref.shape[0]
    live, flip = info[0], info[1]
    for b in range(length // QB):
        rows = pl.ds(place_of(b, own, flip), QB)
        here = pl.ds(b * QB, QB)
        cosine, sine = cos_ref[here, :], sin_ref[here, :]
        query = (turn(q_ref[rows, :], cosine, sine) * HD ** (-0.5)).astype(BF16)
        key = turn(k_ref[rows, :], cosine, sine).astype(BF16)
        value = v_ref[rows, :]
        qo[rows, :] = query
        ko[rows, :] = key
        vo[rows, :] = value.astype(BF16)
        qs[here, :] = query
        ks[here, :] = key
        vt[:, b * QB : (b + 1) * QB] = value.T.astype(BF16)
    for b in range(length // QB):
        rows = pl.ds(place_of(b, own, flip), QB)

        @pl.when(b * QB < live)
        def _():
            allowed = diag_mask(b, live)
            outs = []
            for head in range(2):
                lanes = slice(head * HD, (head + 1) * HD)
                query = only(qs[pl.ds(b * QB, QB), :], head_lanes(head))
                diag = matmul_nt(ks[pl.ds(b * QB, QB), :], query)
                diag = jnp.where(allowed, diag, NEGATIVE)
                top = jnp.max(diag, axis=0, keepdims=True)
                if b:
                    past = matmul_nt(ks[pl.ds(0, b * QB), :], query)
                    top = jnp.maximum(top, jnp.max(past, axis=0, keepdims=True))
                diag = jnp.exp(diag - top)
                total = jnp.sum(diag, axis=0, keepdims=True)
                mixed = matmul(vt[lanes, b * QB : (b + 1) * QB], diag.astype(BF16))
                if b:
                    past = jnp.exp(past - top)
                    total = total + jnp.sum(past, axis=0, keepdims=True)
                    mixed = mixed + matmul(vt[lanes, : b * QB], past.astype(BF16))
                outs.append(mixed / total)
                lo[0, head : head + 1, b * QB : (b + 1) * QB] = top + jnp.log(total)
            ao[rows, :] = jnp.concatenate(outs, axis=0).T.astype(BF16)

        @pl.when(b * QB >= live)
        def _():
            ao[rows, :] = jnp.zeros((QB, LANES), BF16)
            lo[0, 0:2, b * QB : (b + 1) * QB] = jnp.zeros((2, QB), F32)


def attend(qkv, slot, info, cosine, sine, own, length):
    width = qkv.shape[1] // 3
    pairs = width // LANES
    wide = jax.ShapeDtypeStruct((length, width), BF16)

    def column(third):
        return pl.BlockSpec((length, LANES), lambda i, s: (slot, third * pairs + i))

    whole = pl.BlockSpec((length, LANES), lambda i, s: (0, 0))
    out = pl.BlockSpec((length, LANES), lambda i, s: (0, i))
    return pl.pallas_call(
        functools.partial(attend_kernel, own),
        out_shape=[wide] * 4 + [jax.ShapeDtypeStruct((pairs, 8, length), F32)],
        grid_spec=pltpu.PrefetchScalarGridSpec(
            num_scalar_prefetch=1,
            grid=(pairs,),
            in_specs=[column(0), column(1), column(2), whole, whole],
            out_specs=[out] * 4 + [pl.BlockSpec((1, 8, length), lambda i, s: (i, 0, 0))],
            scratch_shapes=[pltpu.VMEM((length, LANES), BF16)] * 2 + [pltpu.VMEM((LANES, length), BF16)],
        ),
        compiler_params=pltpu.CompilerParams(dimension_semantics=("arbitrary",)),
        cost_estimate=pl.CostEstimate(
            flops=8 * length * length * width, bytes_accessed=20 * length * width, transcendentals=0
        ),
        name="attend",
    )(info, qkv, qkv, qkv, cosine, sine)


def attend_back_kernel(
    own, info, q_ref, k_ref, v_ref, a_ref, l_ref, g_ref, cos_ref, sin_ref, out, qs, ks, vs, gs, kt, centre, dq, dk, dv
):
    length = q_ref.shape[0]
    width = out.shape[1] // 3
    live, flip = info[0], info[1]
    pair = pl.program_id(0)
    row = lax.broadcasted_iota(jnp.int32, (8, LANES), 0)
    lane = lax.broadcasted_iota(jnp.int32, (8, LANES), 1)
    sum_head = (lane // HD == row).astype(F32)
    for b in range(length // QB):
        rows = pl.ds(place_of(b, own, flip), QB)
        here = pl.ds(b * QB, QB)
        key = k_ref[rows, :]
        grad = g_ref[rows, :]
        qs[here, :] = q_ref[rows, :]
        ks[here, :] = key
        vs[here, :] = v_ref[rows, :]
        gs[here, :] = grad
        kt[:, b * QB : (b + 1) * QB] = key.astype(F32).T.astype(BF16)
        centre[:, b * QB : (b + 1) * QB] = lax.dot_general(
            sum_head,
            grad.astype(F32) * a_ref[rows, :].astype(F32),
            (((1,), (1,)), ((), ())),
            precision=lax.Precision.HIGHEST,
            preferred_element_type=F32,
        )
    dq[...] = jnp.zeros_like(dq)
    dk[...] = jnp.zeros_like(dk)
    dv[...] = jnp.zeros_like(dv)
    for b in range(length // QB):

        @pl.when(b * QB < live)
        def _():
            here = pl.ds(b * QB, QB)
            columns = slice(b * QB, (b + 1) * QB)
            allowed = diag_mask(b, live)
            diag_p, diag_ds, past_p, past_ds, queries, grads, outs = [], [], [], [], [], [], []
            for head in range(2):
                keep = head_lanes(head)
                lanes = slice(head * HD, (head + 1) * HD)
                query = only(qs[here, :], keep)
                grad = only(gs[here, :], keep)
                log_total = l_ref[0, head : head + 1, columns]
                middle = centre[head : head + 1, columns]
                queries.append(query)
                grads.append(grad)
                prob = jnp.exp(jnp.where(allowed, matmul_nt(ks[here, :], query), NEGATIVE) - log_total)
                slope = (prob * (matmul_nt(vs[here, :], grad) - middle)).astype(BF16)
                diag_p.append(prob.astype(BF16))
                diag_ds.append(slope)
                turned = matmul(kt[lanes, columns], slope)
                if b:
                    before = pl.ds(0, b * QB)
                    prob = jnp.exp(matmul_nt(ks[before, :], query) - log_total)
                    slope = (prob * (matmul_nt(vs[before, :], grad) - middle)).astype(BF16)
                    past_p.append(prob.astype(BF16))
                    past_ds.append(slope)
                    turned = turned + matmul(kt[lanes, : b * QB], slope)
                outs.append(turned)
            queries = jnp.concatenate(queries, axis=0)
            grads = jnp.concatenate(grads, axis=0)
            dk[here, :] += matmul(jnp.concatenate(diag_ds, axis=1), queries)
            dv[here, :] += matmul(jnp.concatenate(diag_p, axis=1), grads)
            if b:
                before = pl.ds(0, b * QB)
                dk[before, :] += matmul(jnp.concatenate(past_ds, axis=1), queries)
                dv[before, :] += matmul(jnp.concatenate(past_p, axis=1), grads)
            dq[here, :] = jnp.concatenate(outs, axis=0).T

    for b in range(length // QB):
        rows = pl.ds(place_of(b, own, flip), QB)
        here = pl.ds(b * QB, QB)
        cosine, sine = cos_ref[here, :], -sin_ref[here, :]

        def columns(third):
            return pl.ds(pl.multiple_of(third * width + pair * LANES, LANES), LANES)

        out[rows, columns(0)] = turn(dq[here, :] * HD ** (-0.5), cosine, sine).astype(BF16)
        out[rows, columns(1)] = turn(dk[here, :], cosine, sine).astype(BF16)
        out[rows, columns(2)] = dv[here, :].astype(BF16)


def attend_back(query, keys, values, mixed, log_total, grad, slot, info, cosine, sine, own, length):
    width = query.shape[1]
    pairs = width // LANES
    block = pl.BlockSpec((length, LANES), lambda i, s: (0, i))
    block_grad = pl.BlockSpec((length, LANES), lambda i, s: (slot, i))
    whole = pl.BlockSpec((length, LANES), lambda i, s: (0, 0))
    return pl.pallas_call(
        functools.partial(attend_back_kernel, own),
        out_shape=jax.ShapeDtypeStruct((length, 3 * width), BF16),
        grid_spec=pltpu.PrefetchScalarGridSpec(
            num_scalar_prefetch=1,
            grid=(pairs,),
            in_specs=[block] * 4
            + [pl.BlockSpec((1, 8, length), lambda i, s: (i, 0, 0)), block_grad, whole, whole],
            out_specs=pl.BlockSpec((length, 3 * width), lambda i, s: (0, 0)),
            scratch_shapes=[pltpu.VMEM((length, LANES), BF16)] * 4
            + [pltpu.VMEM((LANES, length), BF16), pltpu.VMEM((8, length), F32)]
            + [pltpu.VMEM((length, LANES), F32)] * 3,
        ),
        compiler_params=pltpu.CompilerParams(dimension_semantics=("arbitrary",)),
        cost_estimate=pl.CostEstimate(
            flops=20 * length * length * width, bytes_accessed=20 * length * width, transcendentals=0
        ),
        name="attend_back",
    )(info, query, keys, values, mixed, log_total, grad, cosine, sine)


def gate_up_kernel(h_ref, g_ref, u_ref, hid_ref, gate_slope, up_slope):
    gate = matmul(h_ref[...], g_ref[...])
    upward = matmul(h_ref[...], u_ref[...])
    sigma = 1.0 / (1.0 + jnp.exp(-gate))
    silu = gate * sigma
    hid_ref[...] = (silu * upward).astype(BF16)
    gate_slope[...] = (upward * sigma * (1.0 + gate * (1.0 - sigma))).astype(BF16)
    up_slope[...] = silu.astype(BF16)


def tile(extent, most):
    return min(extent, most)


def gate_up(hidden, w_gate, w_up):
    rows, depth = hidden.shape
    width = w_gate.shape[1]
    bm, bn = tile(rows, 512), tile(width, 512)
    weight = pl.BlockSpec((depth, bn), lambda j, i: (0, j))
    out = pl.BlockSpec((bm, bn), lambda j, i: (i, j))
    return pl.pallas_call(
        gate_up_kernel,
        out_shape=[jax.ShapeDtypeStruct((rows, width), BF16)] * 3,
        grid=(width // bn, rows // bm),
        in_specs=[pl.BlockSpec((bm, depth), lambda j, i: (i, 0)), weight, weight],
        out_specs=[out] * 3,
        cost_estimate=pl.CostEstimate(
            flops=4 * rows * depth * width, bytes_accessed=2 * (rows * depth + 2 * depth * width + 3 * rows * width), transcendentals=0
        ),
        name="gate_up",
    )(hidden, w_gate, w_up)


def hidden_back_kernel(g_ref, w_ref, gate_slope, up_slope, gate_out, up_out):
    grad = matmul(g_ref[...], w_ref[...])
    gate_out[...] = (grad * gate_slope[...].astype(F32)).astype(BF16)
    up_out[...] = (grad * up_slope[...].astype(F32)).astype(BF16)


def hidden_back(grad, w_down, gate_slope, up_slope):
    rows, depth = grad.shape
    width = w_down.shape[1]
    bm, bn = tile(rows, 512), tile(width, 512)
    out = pl.BlockSpec((bm, bn), lambda j, i: (i, j))
    return pl.pallas_call(
        hidden_back_kernel,
        out_shape=[jax.ShapeDtypeStruct((rows, width), BF16)] * 2,
        grid=(width // bn, rows // bm),
        in_specs=[
            pl.BlockSpec((bm, depth), lambda j, i: (i, 0)),
            pl.BlockSpec((depth, bn), lambda j, i: (0, j)),
            out,
            out,
        ],
        out_specs=[out] * 2,
        cost_estimate=pl.CostEstimate(
            flops=2 * rows * depth * width, bytes_accessed=2 * (rows * depth + depth * width + 4 * rows * width), transcendentals=0
        ),
        name="hidden_back",
    )(grad, w_down, gate_slope, up_slope)


def two_nt_kernel(a_ref, b_ref, wa_ref, wb_ref, out_ref):
    out_ref[...] = (matmul_nt(a_ref[...], wa_ref[...]) + matmul_nt(b_ref[...], wb_ref[...])).astype(BF16)


def two_nt(first, second, w_first, w_second, start, rows):
    depth = first.shape[1]
    width = w_first.shape[0]
    bm, bn = tile(rows, 512), tile(width, 512)
    left = pl.BlockSpec((bm, depth), lambda j, i: (start // bm + i, 0))
    weight = pl.BlockSpec((bn, depth), lambda j, i: (j, 0))
    return pl.pallas_call(
        two_nt_kernel,
        out_shape=jax.ShapeDtypeStruct((rows, width), BF16),
        grid=(width // bn, rows // bm),
        in_specs=[left, left, weight, weight],
        out_specs=pl.BlockSpec((bm, bn), lambda j, i: (i, j)),
        cost_estimate=pl.CostEstimate(
            flops=4 * rows * depth * width, bytes_accessed=2 * (2 * rows * depth + 2 * depth * width + rows * width), transcendentals=0
        ),
        name="two_nt",
    )(first, second, w_first, w_second)


def hop(value, bit, size):
    return lax.ppermute(value, "tp", [(i, i ^ bit) for i in range(size)])


def bit_orders(size):
    bits = []
    bit = 1
    while bit < size:
        bits.append(bit)
        bit *= 2
    return (bits, bits[::-1])


def gather_tp(halves, size):
    got = []
    for half, order in zip(halves, bit_orders(size)):
        have = {0: half}
        for bit in order:
            for r in sorted(have):
                have[r ^ bit] = hop(have[r], bit, size)
        got.append(have)
    return jnp.concatenate([got[h][r] for r in range(size) for h in range(2)], axis=0)


def scatter_tp(piece, size):
    out = []
    parts = [piece(r) for r in range(size)]
    own = parts[0].shape[0]
    for h, order in enumerate(bit_orders(size)):
        have = {r: parts[r][h * (own // 2) : (h + 1) * (own // 2)] for r in range(size)}
        for step, bit in enumerate(order[::-1]):
            last = step == len(order) - 1
            for r in sorted(have, reverse=True):
                if r & bit:
                    came = hop(have.pop(r), bit, size).astype(F32)
                    total = have[r ^ bit].astype(F32) + came
                    have[r ^ bit] = total if last else total.astype(BF16)
        out.append(have[0].astype(F32))
    return out


def after(value, *others):
    return lax.optimization_barrier((value,) + others)[0]


def scatter_vectors(values):
    axes = ("fsdp", "tp")
    devices = lax.axis_size("fsdp") * lax.axis_size("tp")
    index = lax.axis_index("fsdp") * lax.axis_size("tp") + lax.axis_index("tp")
    bit = devices // 2
    while bit:
        pair = values.reshape(values.shape[0], 2, values.shape[1] // 2)
        mine = (index // bit) % 2
        kept = lax.dynamic_index_in_dim(pair, mine, axis=1, keepdims=False)
        sent = lax.dynamic_index_in_dim(pair, 1 - mine, axis=1, keepdims=False)
        values = kept + lax.ppermute(sent, axes, [(i, i ^ bit) for i in range(devices)])
        bit //= 2
    return values


def split_halves(rows):
    middle = rows.shape[0] // 2
    return [rows[:middle], rows[middle:]]


def per_device(
    tokens, gain_attn, gain_mlp, w_query, w_key, w_value, w_out, w_gate, w_up, w_down, lengths, out_grad
):
    size = lax.axis_size("tp")
    me = lax.axis_index("tp")
    own = tokens.shape[0]
    count = lengths.shape[0]
    group = own * size
    length = group // count
    per_slot = length // own
    my_slot = me // per_slot
    flip = me % per_slot
    head_width = w_query.shape[1]

    def along_fsdp(weight):
        return lax.all_gather(weight, "fsdp", axis=0, tiled=True)

    qkv_full = along_fsdp(jnp.concatenate([w_query, w_key, w_value], axis=1))
    out_full = along_fsdp(w_out)
    gate_full = along_fsdp(w_gate)
    up_full = along_fsdp(w_up)
    down_full = along_fsdp(w_down)

    own_length = lax.dynamic_index_in_dim(lengths, my_slot, keepdims=False)
    places = flip * own + jnp.arange(own, dtype=jnp.int32)
    valid = split_halves((places < own_length).astype(F32)[:, None])
    infos = [
        jnp.stack([lax.dynamic_index_in_dim(lengths, my_slot ^ s, keepdims=False), flip]).astype(jnp.int32)
        for s in range(count)
    ]
    cosine, sine = rotary_tables(length)
    x = [half.astype(F32) for half in split_halves(tokens)]
    scale_one = [inverse_rms(v) for v in x]
    normed_one = [v * s for v, s in zip(x, scale_one)]
    h1 = gather_tp([(n * gain_attn).astype(BF16) for n in normed_one], size)
    grad_rows = [m * g.astype(F32) for m, g in zip(valid, split_halves(out_grad))]

    qkv = matmul(h1, qkv_full)
    saved = {}
    partial = {}
    for s in reversed(range(count)):
        saved[s] = attend(qkv, s, infos[s], cosine, sine, own, length)
        partial[s] = matmul_nt(saved[s][3], out_full).astype(BF16)

    def attn_piece(r):
        s, inside = divmod(r, per_slot)
        return partial[s][inside * own : (inside + 1) * own]

    attn_out = scatter_tp(attn_piece, size)
    middle = [v + a for v, a in zip(x, attn_out)]
    scale_two = [inverse_rms(v) for v in middle]
    normed_two = [v * s for v, s in zip(middle, scale_two)]
    h2 = gather_tp([(n * gain_mlp).astype(BF16) for n in normed_two], size)

    dm_own = after(jnp.concatenate([g.astype(BF16) for g in grad_rows], axis=0), h2)
    dm = jnp.concatenate([dm_own] + [hop(dm_own, r, size) for r in range(1, size)], axis=0)

    hid, gate_slope, up_slope = gate_up(h2, gate_full, up_full)
    down_term = matmul_tn(dm, hid).astype(BF16)
    grad_gate, grad_up = hidden_back(dm, down_full, after(gate_slope, down_term), up_slope)
    half_group = group // 2
    two = {}
    two[1] = two_nt(grad_gate, grad_up, gate_full, up_full, half_group, half_group)
    gate_term = matmul_tn(h2, after(grad_gate, two[1])).astype(BF16)
    two[0] = two_nt(after(grad_gate, gate_term), grad_up, gate_full, up_full, 0, half_group)
    up_term = matmul_tn(h2, after(grad_up, two[0])).astype(BF16)
    mlp = matmul_nt(after(hid, up_term), down_full).astype(BF16)

    def two_piece(r):
        i, inside = divmod(r, size // 2)
        return two[i][inside * own : (inside + 1) * own]

    grad_two = scatter_tp(two_piece, size)
    gain_mlp_term = sum(jnp.sum(g * n, axis=0) for g, n in zip(grad_two, normed_two))
    inner_two = [g * gain_mlp for g in grad_two]
    grad_middle = [
        g + s * (i - n * jnp.mean(i * n, axis=-1, keepdims=True))
        for g, s, i, n in zip(grad_rows, scale_two, inner_two, normed_two)
    ]
    grad_attn = gather_tp([after(g.astype(BF16), gate_term, up_term) for g in grad_middle], size)
    mlp, grad_attn = lax.optimization_barrier((mlp, grad_attn))
    mlp_out = scatter_tp(lambda r: mlp[r * own : (r + 1) * own], size)
    output = jnp.concatenate(
        [(m * (v + o)).astype(BF16) for m, v, o in zip(valid, middle, mlp_out)], axis=0
    )

    grad_mixed = matmul(grad_attn, out_full).astype(BF16)
    grad_qkv = {}
    partial_one = {}
    last = None
    for s in reversed(range(count)):
        query, keys, values, mixed_s, log_total = saved[s]
        if last is not None:
            query = after(query, last)
        grad_qkv[s] = attend_back(query, keys, values, mixed_s, log_total, grad_mixed, s, infos[s], cosine, sine, own, length)
        if s:
            last = partial_one[s] = matmul_nt(grad_qkv[s], qkv_full).astype(BF16)
        if s == count - 1:
            mixed = after(jnp.concatenate([saved[i][3] for i in range(count)], axis=0), last)
            last = out_term = matmul_tn(grad_attn, mixed).astype(BF16)
    grad_all = jnp.concatenate([grad_qkv[s] for s in range(count)], axis=0)
    qkv_term = matmul_tn(h1, grad_all).astype(BF16)
    partial_one[0] = matmul_nt(after(grad_qkv[0], qkv_term), qkv_full).astype(BF16)

    def one_piece(r):
        s, inside = divmod(r, per_slot)
        return partial_one[s][inside * own : (inside + 1) * own]

    grad_one = scatter_tp(one_piece, size)
    gain_attn_term = sum(jnp.sum(g * n, axis=0) for g, n in zip(grad_one, normed_one))
    inner_one = [g * gain_attn for g in grad_one]
    input_grad = jnp.concatenate(
        [
            (m + s * (i - n * jnp.mean(i * n, axis=-1, keepdims=True))).astype(BF16)
            for m, s, i, n in zip(grad_middle, scale_one, inner_one, normed_one)
        ],
        axis=0,
    )

    def back_fsdp(term):
        return lax.psum_scatter(term, "fsdp", scatter_dimension=0, tiled=True).astype(F32)

    down_grad = back_fsdp(down_term)
    gate_grad = back_fsdp(gate_term)
    up_grad = back_fsdp(up_term)
    out_proj_grad = back_fsdp(out_term)
    qkv_grad = back_fsdp(qkv_term)
    gains = scatter_vectors(after(jnp.stack([gain_attn_term, gain_mlp_term]), down_grad, gate_grad, up_grad))
    return (
        output,
        input_grad,
        gains[0],
        gains[1],
        qkv_grad[:, :head_width],
        qkv_grad[:, head_width : 2 * head_width],
        qkv_grad[:, 2 * head_width :],
        out_proj_grad,
        gate_grad,
        up_grad,
        down_grad,
    )


def solution(mesh):
    rows = P(("fsdp", "tp"), None)
    weight = P("fsdp", "tp")
    vector = P(("fsdp", "tp"))
    return jax.shard_map(
        per_device,
        mesh=mesh,
        in_specs=(rows, P(), P()) + (weight,) * 7 + (P("fsdp"), rows),
        out_specs=(rows, rows, vector, vector) + (weight,) * 7,
        check_vma=False,
    )
```

```python
import functools

import jax
import jax.numpy as jnp
from jax import lax
from jax.experimental import pallas as pl
from jax.experimental.pallas import tpu as pltpu
from jax.sharding import PartitionSpec as P


HD = 64
EPS = 1e-05
THETA = 130000.0
NEGATIVE = -1e30
QB = 256
LANES = 128
BF16 = jnp.bfloat16
F32 = jnp.float32


def matmul(left, right):
    return jnp.dot(left, right, preferred_element_type=F32)


def matmul_nt(left, right):
    return lax.dot_general(left, right, (((1,), (1,)), ((), ())), preferred_element_type=F32)


def matmul_tn(left, right):
    return lax.dot_general(left, right, (((0,), (0,)), ((), ())), preferred_element_type=F32)


def inverse_rms(values):
    return lax.rsqrt(jnp.mean(values * values, axis=-1, keepdims=True) + EPS)


def rotary_tables(length):
    half = HD // 2
    places = jnp.arange(length, dtype=F32)[:, None]
    freqs = 1.0 / THETA ** (jnp.arange(half, dtype=F32) * 2.0 / HD)
    angle = places * freqs[None, :]
    cosine, sine = jnp.cos(angle), jnp.sin(angle)
    return (
        jnp.concatenate([cosine] * 4, axis=1),
        jnp.concatenate([-sine, sine, -sine, sine], axis=1),
    )


def turn(field, cosine, sine):
    lane = lax.broadcasted_iota(jnp.int32, (1, LANES), 1)
    swapped = jnp.where((lane & (HD - 1)) < HD // 2, pltpu.roll(field, LANES - HD // 2, 1), pltpu.roll(field, HD // 2, 1))
    return field * cosine + swapped * sine


def head_lanes(head):
    lane = lax.broadcasted_iota(jnp.int32, (1, LANES), 1)
    return lane >= HD if head else lane < HD


def only(values, keep):
    return jnp.where(keep, values, jnp.zeros_like(values))


def place_of(block, own, flip):
    piece, rest = divmod(block * QB, own)
    return pl.multiple_of((piece ^ flip) * own + rest, QB)


def diag_mask(block, live):
    key = lax.broadcasted_iota(jnp.int32, (QB, QB), 0)
    query = lax.broadcasted_iota(jnp.int32, (QB, QB), 1)
    return (key <= query) & (key + block * QB < live)


def attend_kernel(own, info, q_ref, k_ref, v_ref, cos_ref, sin_ref, qo, ko, vo, ao, lo, qs, ks, vt):
    length = q_ref.shape[0]
    live, flip = info[0], info[1]
    for b in range(length // QB):
        rows = pl.ds(place_of(b, own, flip), QB)
        here = pl.ds(b * QB, QB)
        cosine, sine = cos_ref[here, :], sin_ref[here, :]
        query = (turn(q_ref[rows, :], cosine, sine) * HD ** (-0.5)).astype(BF16)
        key = turn(k_ref[rows, :], cosine, sine).astype(BF16)
        value = v_ref[rows, :]
        qo[rows, :] = query
        ko[rows, :] = key
        vo[rows, :] = value.astype(BF16)
        qs[here, :] = query
        ks[here, :] = key
        vt[:, b * QB : (b + 1) * QB] = value.T.astype(BF16)
    for b in range(length // QB):
        rows = pl.ds(place_of(b, own, flip), QB)

        @pl.when(b * QB < live)
        def _():
            allowed = diag_mask(b, live)
            outs = []
            for head in range(2):
                lanes = slice(head * HD, (head + 1) * HD)
                query = only(qs[pl.ds(b * QB, QB), :], head_lanes(head))
                diag = matmul_nt(ks[pl.ds(b * QB, QB), :], query)
                diag = jnp.where(allowed, diag, NEGATIVE)
                top = jnp.max(diag, axis=0, keepdims=True)
                if b:
                    past = matmul_nt(ks[pl.ds(0, b * QB), :], query)
                    top = jnp.maximum(top, jnp.max(past, axis=0, keepdims=True))
                diag = jnp.exp(diag - top)
                total = jnp.sum(diag, axis=0, keepdims=True)
                mixed = matmul(vt[lanes, b * QB : (b + 1) * QB], diag.astype(BF16))
                if b:
                    past = jnp.exp(past - top)
                    total = total + jnp.sum(past, axis=0, keepdims=True)
                    mixed = mixed + matmul(vt[lanes, : b * QB], past.astype(BF16))
                outs.append(mixed / total)
                lo[0, head : head + 1, b * QB : (b + 1) * QB] = top + jnp.log(total)
            ao[rows, :] = jnp.concatenate(outs, axis=0).T.astype(BF16)

        @pl.when(b * QB >= live)
        def _():
            ao[rows, :] = jnp.zeros((QB, LANES), BF16)
            lo[0, 0:2, b * QB : (b + 1) * QB] = jnp.zeros((2, QB), F32)


def attend(qkv, slot, info, cosine, sine, own, length):
    width = qkv.shape[1] // 3
    pairs = width // LANES
    wide = jax.ShapeDtypeStruct((length, width), BF16)

    def column(third):
        return pl.BlockSpec((length, LANES), lambda i, s: (slot, third * pairs + i))

    whole = pl.BlockSpec((length, LANES), lambda i, s: (0, 0))
    out = pl.BlockSpec((length, LANES), lambda i, s: (0, i))
    return pl.pallas_call(
        functools.partial(attend_kernel, own),
        out_shape=[wide] * 4 + [jax.ShapeDtypeStruct((pairs, 8, length), F32)],
        grid_spec=pltpu.PrefetchScalarGridSpec(
            num_scalar_prefetch=1,
            grid=(pairs,),
            in_specs=[column(0), column(1), column(2), whole, whole],
            out_specs=[out] * 4 + [pl.BlockSpec((1, 8, length), lambda i, s: (i, 0, 0))],
            scratch_shapes=[pltpu.VMEM((length, LANES), BF16)] * 2 + [pltpu.VMEM((LANES, length), BF16)],
        ),
        compiler_params=pltpu.CompilerParams(dimension_semantics=("arbitrary",)),
        cost_estimate=pl.CostEstimate(
            flops=8 * length * length * width, bytes_accessed=20 * length * width, transcendentals=0
        ),
        name="attend",
    )(info, qkv, qkv, qkv, cosine, sine)


def attend_back_kernel(
    own, info, q_ref, k_ref, v_ref, a_ref, l_ref, g_ref, cos_ref, sin_ref, out, qs, ks, vs, gs, kt, centre, dq, dk, dv
):
    length = q_ref.shape[0]
    width = out.shape[1] // 3
    live, flip = info[0], info[1]
    pair = pl.program_id(0)
    row = lax.broadcasted_iota(jnp.int32, (8, LANES), 0)
    lane = lax.broadcasted_iota(jnp.int32, (8, LANES), 1)
    sum_head = (lane // HD == row).astype(F32)
    for b in range(length // QB):
        rows = pl.ds(place_of(b, own, flip), QB)
        here = pl.ds(b * QB, QB)
        key = k_ref[rows, :]
        grad = g_ref[rows, :]
        qs[here, :] = q_ref[rows, :]
        ks[here, :] = key
        vs[here, :] = v_ref[rows, :]
        gs[here, :] = grad
        kt[:, b * QB : (b + 1) * QB] = key.astype(F32).T.astype(BF16)
        centre[:, b * QB : (b + 1) * QB] = lax.dot_general(
            sum_head,
            grad.astype(F32) * a_ref[rows, :].astype(F32),
            (((1,), (1,)), ((), ())),
            precision=lax.Precision.HIGHEST,
            preferred_element_type=F32,
        )
    dq[...] = jnp.zeros_like(dq)
    dk[...] = jnp.zeros_like(dk)
    dv[...] = jnp.zeros_like(dv)
    for b in range(length // QB):

        @pl.when(b * QB < live)
        def _():
            here = pl.ds(b * QB, QB)
            columns = slice(b * QB, (b + 1) * QB)
            allowed = diag_mask(b, live)
            diag_p, diag_ds, past_p, past_ds, queries, grads, outs = [], [], [], [], [], [], []
            for head in range(2):
                keep = head_lanes(head)
                lanes = slice(head * HD, (head + 1) * HD)
                query = only(qs[here, :], keep)
                grad = only(gs[here, :], keep)
                log_total = l_ref[0, head : head + 1, columns]
                middle = centre[head : head + 1, columns]
                queries.append(query)
                grads.append(grad)
                prob = jnp.exp(jnp.where(allowed, matmul_nt(ks[here, :], query), NEGATIVE) - log_total)
                slope = (prob * (matmul_nt(vs[here, :], grad) - middle)).astype(BF16)
                diag_p.append(prob.astype(BF16))
                diag_ds.append(slope)
                turned = matmul(kt[lanes, columns], slope)
                if b:
                    before = pl.ds(0, b * QB)
                    prob = jnp.exp(matmul_nt(ks[before, :], query) - log_total)
                    slope = (prob * (matmul_nt(vs[before, :], grad) - middle)).astype(BF16)
                    past_p.append(prob.astype(BF16))
                    past_ds.append(slope)
                    turned = turned + matmul(kt[lanes, : b * QB], slope)
                outs.append(turned)
            queries = jnp.concatenate(queries, axis=0)
            grads = jnp.concatenate(grads, axis=0)
            dk[here, :] += matmul(jnp.concatenate(diag_ds, axis=1), queries)
            dv[here, :] += matmul(jnp.concatenate(diag_p, axis=1), grads)
            if b:
                before = pl.ds(0, b * QB)
                dk[before, :] += matmul(jnp.concatenate(past_ds, axis=1), queries)
                dv[before, :] += matmul(jnp.concatenate(past_p, axis=1), grads)
            dq[here, :] = jnp.concatenate(outs, axis=0).T

    for b in range(length // QB):
        rows = pl.ds(place_of(b, own, flip), QB)
        here = pl.ds(b * QB, QB)
        cosine, sine = cos_ref[here, :], -sin_ref[here, :]

        def columns(third):
            return pl.ds(pl.multiple_of(third * width + pair * LANES, LANES), LANES)

        out[rows, columns(0)] = turn(dq[here, :] * HD ** (-0.5), cosine, sine).astype(BF16)
        out[rows, columns(1)] = turn(dk[here, :], cosine, sine).astype(BF16)
        out[rows, columns(2)] = dv[here, :].astype(BF16)


def attend_back(query, keys, values, mixed, log_total, grad, slot, info, cosine, sine, own, length):
    width = query.shape[1]
    pairs = width // LANES
    block = pl.BlockSpec((length, LANES), lambda i, s: (0, i))
    block_grad = pl.BlockSpec((length, LANES), lambda i, s: (slot, i))
    whole = pl.BlockSpec((length, LANES), lambda i, s: (0, 0))
    return pl.pallas_call(
        functools.partial(attend_back_kernel, own),
        out_shape=jax.ShapeDtypeStruct((length, 3 * width), BF16),
        grid_spec=pltpu.PrefetchScalarGridSpec(
            num_scalar_prefetch=1,
            grid=(pairs,),
            in_specs=[block] * 4
            + [pl.BlockSpec((1, 8, length), lambda i, s: (i, 0, 0)), block_grad, whole, whole],
            out_specs=pl.BlockSpec((length, 3 * width), lambda i, s: (0, 0)),
            scratch_shapes=[pltpu.VMEM((length, LANES), BF16)] * 4
            + [pltpu.VMEM((LANES, length), BF16), pltpu.VMEM((8, length), F32)]
            + [pltpu.VMEM((length, LANES), F32)] * 3,
        ),
        compiler_params=pltpu.CompilerParams(dimension_semantics=("arbitrary",)),
        cost_estimate=pl.CostEstimate(
            flops=20 * length * length * width, bytes_accessed=20 * length * width, transcendentals=0
        ),
        name="attend_back",
    )(info, query, keys, values, mixed, log_total, grad, cosine, sine)


def gate_up_kernel(h_ref, g_ref, u_ref, hid_ref, gate_slope, up_slope):
    gate = matmul(h_ref[...], g_ref[...])
    upward = matmul(h_ref[...], u_ref[...])
    sigma = 1.0 / (1.0 + jnp.exp(-gate))
    silu = gate * sigma
    hid_ref[...] = (silu * upward).astype(BF16)
    gate_slope[...] = (upward * sigma * (1.0 + gate * (1.0 - sigma))).astype(BF16)
    up_slope[...] = silu.astype(BF16)


def tile(extent, most):
    return min(extent, most)


def gate_up(hidden, w_gate, w_up):
    rows, depth = hidden.shape
    width = w_gate.shape[1]
    bm, bn = tile(rows, 512), tile(width, 512)
    weight = pl.BlockSpec((depth, bn), lambda j, i: (0, j))
    out = pl.BlockSpec((bm, bn), lambda j, i: (i, j))
    return pl.pallas_call(
        gate_up_kernel,
        out_shape=[jax.ShapeDtypeStruct((rows, width), BF16)] * 3,
        grid=(width // bn, rows // bm),
        in_specs=[pl.BlockSpec((bm, depth), lambda j, i: (i, 0)), weight, weight],
        out_specs=[out] * 3,
        cost_estimate=pl.CostEstimate(
            flops=4 * rows * depth * width, bytes_accessed=2 * (rows * depth + 2 * depth * width + 3 * rows * width), transcendentals=0
        ),
        name="gate_up",
    )(hidden, w_gate, w_up)


def hidden_back_kernel(g_ref, w_ref, gate_slope, up_slope, gate_out, up_out):
    grad = matmul(g_ref[...], w_ref[...])
    gate_out[...] = (grad * gate_slope[...].astype(F32)).astype(BF16)
    up_out[...] = (grad * up_slope[...].astype(F32)).astype(BF16)


def hidden_back(grad, w_down, gate_slope, up_slope):
    rows, depth = grad.shape
    width = w_down.shape[1]
    bm, bn = tile(rows, 512), tile(width, 512)
    out = pl.BlockSpec((bm, bn), lambda j, i: (i, j))
    return pl.pallas_call(
        hidden_back_kernel,
        out_shape=[jax.ShapeDtypeStruct((rows, width), BF16)] * 2,
        grid=(width // bn, rows // bm),
        in_specs=[
            pl.BlockSpec((bm, depth), lambda j, i: (i, 0)),
            pl.BlockSpec((depth, bn), lambda j, i: (0, j)),
            out,
            out,
        ],
        out_specs=[out] * 2,
        cost_estimate=pl.CostEstimate(
            flops=2 * rows * depth * width, bytes_accessed=2 * (rows * depth + depth * width + 4 * rows * width), transcendentals=0
        ),
        name="hidden_back",
    )(grad, w_down, gate_slope, up_slope)


def two_nt_kernel(a_ref, b_ref, wa_ref, wb_ref, out_ref):
    out_ref[...] = (matmul_nt(a_ref[...], wa_ref[...]) + matmul_nt(b_ref[...], wb_ref[...])).astype(BF16)


def two_nt(first, second, w_first, w_second, start, rows):
    depth = first.shape[1]
    width = w_first.shape[0]
    bm, bn = tile(rows, 512), tile(width, 512)
    left = pl.BlockSpec((bm, depth), lambda j, i: (start // bm + i, 0))
    weight = pl.BlockSpec((bn, depth), lambda j, i: (j, 0))
    return pl.pallas_call(
        two_nt_kernel,
        out_shape=jax.ShapeDtypeStruct((rows, width), BF16),
        grid=(width // bn, rows // bm),
        in_specs=[left, left, weight, weight],
        out_specs=pl.BlockSpec((bm, bn), lambda j, i: (i, j)),
        cost_estimate=pl.CostEstimate(
            flops=4 * rows * depth * width, bytes_accessed=2 * (2 * rows * depth + 2 * depth * width + rows * width), transcendentals=0
        ),
        name="two_nt",
    )(first, second, w_first, w_second)


def hop(value, bit, size):
    return lax.ppermute(value, "tp", [(i, i ^ bit) for i in range(size)])


def bit_orders(size):
    bits = []
    bit = 1
    while bit < size:
        bits.append(bit)
        bit *= 2
    return (bits, bits[::-1])


def gather_tp(halves, size, hold=None):
    got = []
    for half, order in zip(halves, bit_orders(size)):
        have = {0: half}
        for bit in order:
            for r in sorted(have):
                sent = have[r] if hold is None or not r else after(have[r], hold)
                have[r ^ bit] = hop(sent, bit, size)
        got.append(have)
    return [got[h][r] for r in range(size) for h in range(2)]


def rows_of(pieces):
    return jnp.concatenate(pieces, axis=0)


def scatter_tp(piece, size, settle=False):
    out = []
    parts = [piece(r) for r in range(size)]
    own = parts[0].shape[0]
    for h, order in enumerate(bit_orders(size)):
        have = {r: parts[r][h * (own // 2) : (h + 1) * (own // 2)] for r in range(size)}
        for step, bit in enumerate(order[::-1]):
            for r in sorted(have, reverse=True):
                if r & bit:
                    came = hop(have.pop(r), bit, size).astype(F32)
                    total = have[r ^ bit].astype(F32) + came
                    if r ^ bit or (settle and step < len(order) - 1):
                        total = lax.optimization_barrier(total.astype(BF16))
                    have[r ^ bit] = total
        out.append(have[0].astype(F32))
    return out


def after(value, *others):
    return lax.optimization_barrier((value,) + others)[0]


def scatter_vectors(values):
    sizes = {axis: lax.axis_size(axis) for axis in ("fsdp", "tp")}
    values = values.reshape(values.shape[0], sizes["fsdp"], sizes["tp"], -1)
    for axis, dim in (("tp", 2), ("fsdp", 1)):
        size, me = sizes[axis], lax.axis_index(axis)
        total = lax.dynamic_index_in_dim(values, me, axis=dim, keepdims=False)
        for r in range(1, size):
            sent = lax.dynamic_index_in_dim(values, me ^ r, axis=dim, keepdims=False)
            total = total + lax.ppermute(sent, axis, [(i, i ^ r) for i in range(size)])
        values = total
    return values


def split_halves(rows):
    middle = rows.shape[0] // 2
    return [rows[:middle], rows[middle:]]


def per_device(
    tokens, gain_attn, gain_mlp, w_query, w_key, w_value, w_out, w_gate, w_up, w_down, lengths, out_grad
):
    size = lax.axis_size("tp")
    me = lax.axis_index("tp")
    own = tokens.shape[0]
    count = lengths.shape[0]
    group = own * size
    length = group // count
    per_slot = length // own
    my_slot = me // per_slot
    flip = me % per_slot
    head_width = w_query.shape[1]

    def along_fsdp(weight):
        return lax.all_gather(weight, "fsdp", axis=0, tiled=True)

    qkv_full = along_fsdp(jnp.concatenate([w_query, w_key, w_value], axis=1))
    out_full = along_fsdp(w_out)
    gate_full = along_fsdp(w_gate)
    up_full = along_fsdp(w_up)
    down_full = along_fsdp(w_down)

    def back_fsdp(term):
        return lax.psum_scatter(term, "fsdp", scatter_dimension=0, tiled=True).astype(F32)

    own_length = lax.dynamic_index_in_dim(lengths, my_slot, keepdims=False)
    places = flip * own + jnp.arange(own, dtype=jnp.int32)
    valid = split_halves((places < own_length).astype(F32)[:, None])
    infos = [
        jnp.stack([lax.dynamic_index_in_dim(lengths, my_slot ^ s, keepdims=False), flip]).astype(jnp.int32)
        for s in range(count)
    ]
    cosine, sine = rotary_tables(length)
    x = [half.astype(F32) for half in split_halves(tokens)]
    scale_one = [inverse_rms(v) for v in x]
    normed_one = [v * s for v, s in zip(x, scale_one)]
    h1_pieces = gather_tp([(n * gain_attn).astype(BF16) for n in normed_one], size)
    h1_slot = [rows_of(h1_pieces[2 * per_slot * s : 2 * per_slot * (s + 1)]) for s in range(count)]
    grad_rows = [m * g.astype(F32) for m, g in zip(valid, split_halves(out_grad))]

    qkv = [matmul(h1_slot[0], qkv_full)]
    for s in range(1, count):
        qkv.append(matmul(after(h1_slot[s], qkv[-1]), qkv_full))
    saved = {}
    partial = {}
    for s in reversed(range(count)):
        saved[s] = attend(qkv[s], 0, infos[s], cosine, sine, own, length)
        partial[s] = matmul_nt(saved[s][3], out_full).astype(BF16)

    def attn_piece(r):
        s, inside = divmod(r, per_slot)
        return partial[s][inside * own : (inside + 1) * own]

    attn_out = scatter_tp(attn_piece, size)
    middle = [v + a for v, a in zip(x, attn_out)]
    scale_two = [inverse_rms(v) for v in middle]
    normed_two = [v * s for v, s in zip(middle, scale_two)]
    h2 = rows_of(gather_tp([(n * gain_mlp).astype(BF16) for n in normed_two], size))

    dm = rows_of(gather_tp([after(g.astype(BF16), h1_slot[-1]) for g in grad_rows], size, h2))

    hid, gate_slope, up_slope = gate_up(h2, gate_full, up_full)
    down_term = matmul_tn(dm, hid).astype(BF16)
    grad_gate, grad_up = hidden_back(dm, down_full, after(gate_slope, down_term), up_slope)
    half_group = group // 2
    two = {}
    two[1] = two_nt(grad_gate, grad_up, gate_full, up_full, half_group, half_group)
    two[0] = two_nt(after(grad_gate, two[1]), grad_up, gate_full, up_full, 0, half_group)
    gate_term = matmul_tn(h2, after(grad_gate, two[0])).astype(BF16)
    up_term = matmul_tn(h2, after(grad_up, gate_term)).astype(BF16)
    mlp = matmul_nt(after(hid, up_term), down_full).astype(BF16)

    def two_piece(r):
        i, inside = divmod(r, size // 2)
        return two[i][inside * own : (inside + 1) * own]

    grad_two = scatter_tp(two_piece, size)
    gain_mlp_term = sum(jnp.sum(g * n, axis=0) for g, n in zip(grad_two, normed_two))
    inner_two = [g * gain_mlp for g in grad_two]
    grad_middle = [
        g + s * (i - n * jnp.mean(i * n, axis=-1, keepdims=True))
        for g, s, i, n in zip(grad_rows, scale_two, inner_two, normed_two)
    ]
    grad_attn = rows_of(gather_tp([after(g.astype(BF16), gate_term, up_term) for g in grad_middle], size))
    down_grad = back_fsdp(down_term)
    gate_grad = back_fsdp(gate_term)
    up_grad = back_fsdp(up_term)
    mlp, grad_attn, down_grad, gate_grad = lax.optimization_barrier((mlp, grad_attn, down_grad, gate_grad))
    mlp_out = scatter_tp(lambda r: mlp[r * own : (r + 1) * own], size, settle=True)
    output = jnp.concatenate(
        [(m * (v + o)).astype(BF16) for m, v, o in zip(valid, middle, mlp_out)], axis=0
    )

    grad_mixed = matmul(grad_attn, out_full).astype(BF16)
    grad_qkv = {}
    partial_one = {}
    last = None
    for s in reversed(range(count)):
        query, keys, values, mixed_s, log_total = saved[s]
        if last is not None:
            query = after(query, last)
        grad_qkv[s] = attend_back(query, keys, values, mixed_s, log_total, grad_mixed, s, infos[s], cosine, sine, own, length)
        if s:
            last = partial_one[s] = matmul_nt(grad_qkv[s], qkv_full).astype(BF16)
        if s == count - 1:
            mixed = after(jnp.concatenate([saved[i][3] for i in range(count)], axis=0), last)
            last = out_term = matmul_tn(grad_attn, mixed).astype(BF16)
    grad_all = jnp.concatenate([grad_qkv[s] for s in range(count)], axis=0)
    qkv_term = matmul_tn(rows_of(h1_slot), grad_all).astype(BF16)
    partial_one[0] = matmul_nt(after(grad_qkv[0], qkv_term, up_grad), qkv_full).astype(BF16)

    def one_piece(r):
        s, inside = divmod(r, per_slot)
        return partial_one[s][inside * own : (inside + 1) * own]

    grad_one = scatter_tp(one_piece, size)
    gain_attn_term = sum(jnp.sum(g * n, axis=0) for g, n in zip(grad_one, normed_one))
    inner_one = [g * gain_attn for g in grad_one]
    input_grad = jnp.concatenate(
        [
            (m + s * (i - n * jnp.mean(i * n, axis=-1, keepdims=True))).astype(BF16)
            for m, s, i, n in zip(grad_middle, scale_one, inner_one, normed_one)
        ],
        axis=0,
    )

    out_proj_grad = back_fsdp(out_term)
    qkv_grad = back_fsdp(qkv_term)
    gains = scatter_vectors(jnp.stack([gain_attn_term, gain_mlp_term]))
    return (
        output,
        input_grad,
        gains[0],
        gains[1],
        qkv_grad[:, :head_width],
        qkv_grad[:, head_width : 2 * head_width],
        qkv_grad[:, 2 * head_width :],
        out_proj_grad,
        gate_grad,
        up_grad,
        down_grad,
    )


def solution(mesh):
    rows = P(("fsdp", "tp"), None)
    weight = P("fsdp", "tp")
    vector = P(("fsdp", "tp"))
    return jax.shard_map(
        per_device,
        mesh=mesh,
        in_specs=(rows, P(), P()) + (weight,) * 7 + (P("fsdp"), rows),
        out_specs=(rows, rows, vector, vector) + (weight,) * 7,
        check_vma=False,
    )
```

```python
import functools

import jax
import jax.numpy as jnp
from jax import lax
from jax.experimental import pallas as pl
from jax.experimental.pallas import tpu as pltpu
from jax.sharding import PartitionSpec as P


HD = 64
EPS = 1e-05
THETA = 130000.0
NEGATIVE = -1e30
QB = 256
LANES = 128
BF16 = jnp.bfloat16
F32 = jnp.float32


def matmul(left, right):
    return jnp.dot(left, right, preferred_element_type=F32)


def matmul_nt(left, right):
    return lax.dot_general(left, right, (((1,), (1,)), ((), ())), preferred_element_type=F32)


def matmul_tn(left, right):
    return lax.dot_general(left, right, (((0,), (0,)), ((), ())), preferred_element_type=F32)


def inverse_rms(values):
    return lax.rsqrt(jnp.mean(values * values, axis=-1, keepdims=True) + EPS)


def rotary_tables(length):
    half = HD // 2
    places = jnp.arange(length, dtype=F32)[:, None]
    freqs = 1.0 / THETA ** (jnp.arange(half, dtype=F32) * 2.0 / HD)
    angle = places * freqs[None, :]
    cosine, sine = jnp.cos(angle), jnp.sin(angle)
    return (
        jnp.concatenate([cosine] * 4, axis=1),
        jnp.concatenate([-sine, sine, -sine, sine], axis=1),
    )


def turn(field, cosine, sine):
    lane = lax.broadcasted_iota(jnp.int32, (1, LANES), 1)
    swapped = jnp.where((lane & (HD - 1)) < HD // 2, pltpu.roll(field, LANES - HD // 2, 1), pltpu.roll(field, HD // 2, 1))
    return field * cosine + swapped * sine


def head_lanes(head):
    lane = lax.broadcasted_iota(jnp.int32, (1, LANES), 1)
    return lane >= HD if head else lane < HD


def only(values, keep):
    return jnp.where(keep, values, jnp.zeros_like(values))


def place_of(block, own, flip):
    piece, rest = divmod(block * QB, own)
    return pl.multiple_of((piece ^ flip) * own + rest, QB)


def diag_mask(block, live):
    key = lax.broadcasted_iota(jnp.int32, (QB, QB), 0)
    query = lax.broadcasted_iota(jnp.int32, (QB, QB), 1)
    return (key <= query) & (key + block * QB < live)


def attend_kernel(own, info, q_ref, k_ref, v_ref, cos_ref, sin_ref, qo, ko, vo, ao, lo, qs, ks, vt):
    length = q_ref.shape[0]
    live, flip = info[0], info[1]
    for b in range(length // QB):
        rows = pl.ds(place_of(b, own, flip), QB)
        here = pl.ds(b * QB, QB)
        cosine, sine = cos_ref[here, :], sin_ref[here, :]
        query = (turn(q_ref[rows, :], cosine, sine) * HD ** (-0.5)).astype(BF16)
        key = turn(k_ref[rows, :], cosine, sine).astype(BF16)
        value = v_ref[rows, :]
        qo[rows, :] = query
        ko[rows, :] = key
        vo[rows, :] = value.astype(BF16)
        qs[here, :] = query
        ks[here, :] = key
        vt[:, b * QB : (b + 1) * QB] = value.T.astype(BF16)
    for b in range(length // QB):
        rows = pl.ds(place_of(b, own, flip), QB)

        @pl.when(b * QB < live)
        def _():
            allowed = diag_mask(b, live)
            outs = []
            for head in range(2):
                lanes = slice(head * HD, (head + 1) * HD)
                query = only(qs[pl.ds(b * QB, QB), :], head_lanes(head))
                diag = matmul_nt(ks[pl.ds(b * QB, QB), :], query)
                diag = jnp.where(allowed, diag, NEGATIVE)
                top = jnp.max(diag, axis=0, keepdims=True)
                if b:
                    past = matmul_nt(ks[pl.ds(0, b * QB), :], query)
                    top = jnp.maximum(top, jnp.max(past, axis=0, keepdims=True))
                diag = jnp.exp(diag - top)
                total = jnp.sum(diag, axis=0, keepdims=True)
                mixed = matmul(vt[lanes, b * QB : (b + 1) * QB], diag.astype(BF16))
                if b:
                    past = jnp.exp(past - top)
                    total = total + jnp.sum(past, axis=0, keepdims=True)
                    mixed = mixed + matmul(vt[lanes, : b * QB], past.astype(BF16))
                outs.append(mixed / total)
                lo[0, head : head + 1, b * QB : (b + 1) * QB] = top + jnp.log(total)
            ao[rows, :] = jnp.concatenate(outs, axis=0).T.astype(BF16)

        @pl.when(b * QB >= live)
        def _():
            ao[rows, :] = jnp.zeros((QB, LANES), BF16)
            lo[0, 0:2, b * QB : (b + 1) * QB] = jnp.zeros((2, QB), F32)


def attend(qkv, slot, info, cosine, sine, own, length):
    width = qkv.shape[1] // 3
    pairs = width // LANES
    wide = jax.ShapeDtypeStruct((length, width), BF16)

    def column(third):
        return pl.BlockSpec((length, LANES), lambda i, s: (slot, third * pairs + i))

    whole = pl.BlockSpec((length, LANES), lambda i, s: (0, 0))
    out = pl.BlockSpec((length, LANES), lambda i, s: (0, i))
    return pl.pallas_call(
        functools.partial(attend_kernel, own),
        out_shape=[wide] * 4 + [jax.ShapeDtypeStruct((pairs, 8, length), F32)],
        grid_spec=pltpu.PrefetchScalarGridSpec(
            num_scalar_prefetch=1,
            grid=(pairs,),
            in_specs=[column(0), column(1), column(2), whole, whole],
            out_specs=[out] * 4 + [pl.BlockSpec((1, 8, length), lambda i, s: (i, 0, 0))],
            scratch_shapes=[pltpu.VMEM((length, LANES), BF16)] * 2 + [pltpu.VMEM((LANES, length), BF16)],
        ),
        compiler_params=pltpu.CompilerParams(dimension_semantics=("arbitrary",)),
        cost_estimate=pl.CostEstimate(
            flops=8 * length * length * width, bytes_accessed=20 * length * width, transcendentals=0
        ),
        name="attend",
    )(info, qkv, qkv, qkv, cosine, sine)


def attend_back_kernel(
    own, info, q_ref, k_ref, v_ref, a_ref, l_ref, g_ref, cos_ref, sin_ref, out, qs, ks, vs, gs, kt, centre, dq, dk, dv
):
    length = q_ref.shape[0]
    width = out.shape[1] // 3
    live, flip = info[0], info[1]
    pair = pl.program_id(0)
    row = lax.broadcasted_iota(jnp.int32, (8, LANES), 0)
    lane = lax.broadcasted_iota(jnp.int32, (8, LANES), 1)
    sum_head = (lane // HD == row).astype(F32)
    for b in range(length // QB):
        rows = pl.ds(place_of(b, own, flip), QB)
        here = pl.ds(b * QB, QB)
        key = k_ref[rows, :]
        grad = g_ref[rows, :]
        qs[here, :] = q_ref[rows, :]
        ks[here, :] = key
        vs[here, :] = v_ref[rows, :]
        gs[here, :] = grad
        kt[:, b * QB : (b + 1) * QB] = key.astype(F32).T.astype(BF16)
        centre[:, b * QB : (b + 1) * QB] = lax.dot_general(
            sum_head,
            grad.astype(F32) * a_ref[rows, :].astype(F32),
            (((1,), (1,)), ((), ())),
            precision=lax.Precision.HIGHEST,
            preferred_element_type=F32,
        )
    dq[...] = jnp.zeros_like(dq)
    dk[...] = jnp.zeros_like(dk)
    dv[...] = jnp.zeros_like(dv)
    for b in range(length // QB):

        @pl.when(b * QB < live)
        def _():
            here = pl.ds(b * QB, QB)
            columns = slice(b * QB, (b + 1) * QB)
            allowed = diag_mask(b, live)
            diag_p, diag_ds, past_p, past_ds, queries, grads, outs = [], [], [], [], [], [], []
            for head in range(2):
                keep = head_lanes(head)
                lanes = slice(head * HD, (head + 1) * HD)
                query = only(qs[here, :], keep)
                grad = only(gs[here, :], keep)
                log_total = l_ref[0, head : head + 1, columns]
                middle = centre[head : head + 1, columns]
                queries.append(query)
                grads.append(grad)
                prob = jnp.exp(jnp.where(allowed, matmul_nt(ks[here, :], query), NEGATIVE) - log_total)
                slope = (prob * (matmul_nt(vs[here, :], grad) - middle)).astype(BF16)
                diag_p.append(prob.astype(BF16))
                diag_ds.append(slope)
                turned = matmul(kt[lanes, columns], slope)
                if b:
                    before = pl.ds(0, b * QB)
                    prob = jnp.exp(matmul_nt(ks[before, :], query) - log_total)
                    slope = (prob * (matmul_nt(vs[before, :], grad) - middle)).astype(BF16)
                    past_p.append(prob.astype(BF16))
                    past_ds.append(slope)
                    turned = turned + matmul(kt[lanes, : b * QB], slope)
                outs.append(turned)
            queries = jnp.concatenate(queries, axis=0)
            grads = jnp.concatenate(grads, axis=0)
            dk[here, :] += matmul(jnp.concatenate(diag_ds, axis=1), queries)
            dv[here, :] += matmul(jnp.concatenate(diag_p, axis=1), grads)
            if b:
                before = pl.ds(0, b * QB)
                dk[before, :] += matmul(jnp.concatenate(past_ds, axis=1), queries)
                dv[before, :] += matmul(jnp.concatenate(past_p, axis=1), grads)
            dq[here, :] = jnp.concatenate(outs, axis=0).T

    for b in range(length // QB):
        rows = pl.ds(place_of(b, own, flip), QB)
        here = pl.ds(b * QB, QB)
        cosine, sine = cos_ref[here, :], -sin_ref[here, :]

        def columns(third):
            return pl.ds(pl.multiple_of(third * width + pair * LANES, LANES), LANES)

        out[rows, columns(0)] = turn(dq[here, :] * HD ** (-0.5), cosine, sine).astype(BF16)
        out[rows, columns(1)] = turn(dk[here, :], cosine, sine).astype(BF16)
        out[rows, columns(2)] = dv[here, :].astype(BF16)


def attend_back(query, keys, values, mixed, log_total, grad, slot, info, cosine, sine, own, length):
    width = query.shape[1]
    pairs = width // LANES
    block = pl.BlockSpec((length, LANES), lambda i, s: (0, i))
    block_grad = pl.BlockSpec((length, LANES), lambda i, s: (slot, i))
    whole = pl.BlockSpec((length, LANES), lambda i, s: (0, 0))
    return pl.pallas_call(
        functools.partial(attend_back_kernel, own),
        out_shape=jax.ShapeDtypeStruct((length, 3 * width), BF16),
        grid_spec=pltpu.PrefetchScalarGridSpec(
            num_scalar_prefetch=1,
            grid=(pairs,),
            in_specs=[block] * 4
            + [pl.BlockSpec((1, 8, length), lambda i, s: (i, 0, 0)), block_grad, whole, whole],
            out_specs=pl.BlockSpec((length, 3 * width), lambda i, s: (0, 0)),
            scratch_shapes=[pltpu.VMEM((length, LANES), BF16)] * 4
            + [pltpu.VMEM((LANES, length), BF16), pltpu.VMEM((8, length), F32)]
            + [pltpu.VMEM((length, LANES), F32)] * 3,
        ),
        compiler_params=pltpu.CompilerParams(dimension_semantics=("arbitrary",)),
        cost_estimate=pl.CostEstimate(
            flops=20 * length * length * width, bytes_accessed=20 * length * width, transcendentals=0
        ),
        name="attend_back",
    )(info, query, keys, values, mixed, log_total, grad, cosine, sine)


def gate_up_kernel(h_ref, g_ref, u_ref, hid_ref, gate_slope, up_slope):
    gate = matmul(h_ref[...], g_ref[...])
    upward = matmul(h_ref[...], u_ref[...])
    sigma = 1.0 / (1.0 + jnp.exp(-gate))
    silu = gate * sigma
    hid_ref[...] = (silu * upward).astype(BF16)
    gate_slope[...] = (upward * sigma * (1.0 + gate * (1.0 - sigma))).astype(BF16)
    up_slope[...] = silu.astype(BF16)


def tile(extent, most):
    return min(extent, most)


def gate_up(hidden, w_gate, w_up):
    rows, depth = hidden.shape
    width = w_gate.shape[1]
    bm, bn = tile(rows, 512), tile(width, 512)
    weight = pl.BlockSpec((depth, bn), lambda j, i: (0, j))
    out = pl.BlockSpec((bm, bn), lambda j, i: (i, j))
    return pl.pallas_call(
        gate_up_kernel,
        out_shape=[jax.ShapeDtypeStruct((rows, width), BF16)] * 3,
        grid=(width // bn, rows // bm),
        in_specs=[pl.BlockSpec((bm, depth), lambda j, i: (i, 0)), weight, weight],
        out_specs=[out] * 3,
        cost_estimate=pl.CostEstimate(
            flops=4 * rows * depth * width, bytes_accessed=2 * (rows * depth + 2 * depth * width + 3 * rows * width), transcendentals=0
        ),
        name="gate_up",
    )(hidden, w_gate, w_up)


def hidden_back_kernel(g_ref, w_ref, gate_slope, up_slope, gate_out, up_out):
    grad = matmul(g_ref[...], w_ref[...])
    gate_out[...] = (grad * gate_slope[...].astype(F32)).astype(BF16)
    up_out[...] = (grad * up_slope[...].astype(F32)).astype(BF16)


def hidden_back(grad, w_down, gate_slope, up_slope):
    rows, depth = grad.shape
    width = w_down.shape[1]
    bm, bn = tile(rows, 512), tile(width, 512)
    out = pl.BlockSpec((bm, bn), lambda j, i: (i, j))
    return pl.pallas_call(
        hidden_back_kernel,
        out_shape=[jax.ShapeDtypeStruct((rows, width), BF16)] * 2,
        grid=(width // bn, rows // bm),
        in_specs=[
            pl.BlockSpec((bm, depth), lambda j, i: (i, 0)),
            pl.BlockSpec((depth, bn), lambda j, i: (0, j)),
            out,
            out,
        ],
        out_specs=[out] * 2,
        cost_estimate=pl.CostEstimate(
            flops=2 * rows * depth * width, bytes_accessed=2 * (rows * depth + depth * width + 4 * rows * width), transcendentals=0
        ),
        name="hidden_back",
    )(grad, w_down, gate_slope, up_slope)


def two_nt_kernel(a_ref, b_ref, wa_ref, wb_ref, out_ref):
    out_ref[...] = (matmul_nt(a_ref[...], wa_ref[...]) + matmul_nt(b_ref[...], wb_ref[...])).astype(BF16)


def two_nt(first, second, w_first, w_second, start, rows):
    depth = first.shape[1]
    width = w_first.shape[0]
    bm, bn = tile(rows, 512), tile(width, 512)
    left = pl.BlockSpec((bm, depth), lambda j, i: (start // bm + i, 0))
    weight = pl.BlockSpec((bn, depth), lambda j, i: (j, 0))
    return pl.pallas_call(
        two_nt_kernel,
        out_shape=jax.ShapeDtypeStruct((rows, width), BF16),
        grid=(width // bn, rows // bm),
        in_specs=[left, left, weight, weight],
        out_specs=pl.BlockSpec((bm, bn), lambda j, i: (i, j)),
        cost_estimate=pl.CostEstimate(
            flops=4 * rows * depth * width, bytes_accessed=2 * (2 * rows * depth + 2 * depth * width + rows * width), transcendentals=0
        ),
        name="two_nt",
    )(first, second, w_first, w_second)


def hop(value, bit, size):
    return lax.ppermute(value, "tp", [(i, i ^ bit) for i in range(size)])


def bit_orders(size):
    bits = []
    bit = 1
    while bit < size:
        bits.append(bit)
        bit *= 2
    return (bits, bits[::-1])


def gather_tp(halves, size, hold=None):
    got = []
    for half, order in zip(halves, bit_orders(size)):
        have = {0: half}
        for bit in order:
            for r in sorted(have):
                sent = have[r] if hold is None or not r else after(have[r], hold)
                have[r ^ bit] = hop(sent, bit, size)
        got.append(have)
    return [got[h][r] for r in range(size) for h in range(2)]


def rows_of(pieces):
    return jnp.concatenate(pieces, axis=0)


def scatter_tp(piece, size, settle=False):
    out = []
    parts = [piece(r) for r in range(size)]
    own = parts[0].shape[0]
    for h, order in enumerate(bit_orders(size)):
        have = {r: parts[r][h * (own // 2) : (h + 1) * (own // 2)] for r in range(size)}
        for step, bit in enumerate(order[::-1]):
            for r in sorted(have, reverse=True):
                if r & bit:
                    came = hop(have.pop(r), bit, size).astype(F32)
                    total = have[r ^ bit].astype(F32) + came
                    if r ^ bit or (settle and step < len(order) - 1):
                        total = lax.optimization_barrier(total.astype(BF16))
                    have[r ^ bit] = total
        out.append(have[0].astype(F32))
    return out


def after(value, *others):
    return lax.optimization_barrier((value,) + others)[0]


def scatter_vectors(values):
    sizes = {axis: lax.axis_size(axis) for axis in ("fsdp", "tp")}
    values = values.reshape(values.shape[0], sizes["fsdp"], sizes["tp"], -1)
    for axis in ("fsdp", "tp"):
        dim = 1
        size, me = sizes[axis], lax.axis_index(axis)
        total = lax.dynamic_index_in_dim(values, me, axis=dim, keepdims=False)
        for r in range(1, size):
            sent = lax.dynamic_index_in_dim(values, me ^ r, axis=dim, keepdims=False)
            total = total + lax.ppermute(sent, axis, [(i, i ^ r) for i in range(size)])
        values = total
    return values


def split_halves(rows):
    middle = rows.shape[0] // 2
    return [rows[:middle], rows[middle:]]


def per_device(
    tokens, gain_attn, gain_mlp, w_query, w_key, w_value, w_out, w_gate, w_up, w_down, lengths, out_grad
):
    size = lax.axis_size("tp")
    me = lax.axis_index("tp")
    own = tokens.shape[0]
    count = lengths.shape[0]
    group = own * size
    length = group // count
    per_slot = length // own
    my_slot = me // per_slot
    flip = me % per_slot
    head_width = w_query.shape[1]

    def along_fsdp(weight):
        return lax.all_gather(weight, "fsdp", axis=0, tiled=True)

    qkv_full = along_fsdp(jnp.concatenate([w_query, w_key, w_value], axis=1))
    out_full = along_fsdp(w_out)
    gate_full = along_fsdp(w_gate)
    up_full = along_fsdp(w_up)
    down_full = along_fsdp(w_down)

    def back_fsdp(term):
        return lax.psum_scatter(term, "fsdp", scatter_dimension=0, tiled=True).astype(F32)

    own_length = lax.dynamic_index_in_dim(lengths, my_slot, keepdims=False)
    places = flip * own + jnp.arange(own, dtype=jnp.int32)
    valid = split_halves((places < own_length).astype(F32)[:, None])
    infos = [
        jnp.stack([lax.dynamic_index_in_dim(lengths, my_slot ^ s, keepdims=False), flip]).astype(jnp.int32)
        for s in range(count)
    ]
    cosine, sine = rotary_tables(length)
    x = [half.astype(F32) for half in split_halves(tokens)]
    scale_one = [inverse_rms(v) for v in x]
    normed_one = [v * s for v, s in zip(x, scale_one)]
    h1_pieces = gather_tp([(n * gain_attn).astype(BF16) for n in normed_one], size)
    h1_slot = [rows_of(h1_pieces[2 * per_slot * s : 2 * per_slot * (s + 1)]) for s in range(count)]
    grad_rows = [m * g.astype(F32) for m, g in zip(valid, split_halves(out_grad))]

    qkv = [matmul(h1_slot[0], qkv_full)]
    for s in range(1, count):
        qkv.append(matmul(after(h1_slot[s], qkv[-1]), qkv_full))
    saved = {}
    partial = {}
    for s in reversed(range(count)):
        saved[s] = attend(qkv[s], 0, infos[s], cosine, sine, own, length)
        partial[s] = matmul_nt(saved[s][3], out_full).astype(BF16)

    def attn_piece(r):
        s, inside = divmod(r, per_slot)
        return partial[s][inside * own : (inside + 1) * own]

    attn_out = scatter_tp(attn_piece, size)
    middle = [v + a for v, a in zip(x, attn_out)]
    scale_two = [inverse_rms(v) for v in middle]
    normed_two = [v * s for v, s in zip(middle, scale_two)]
    h2 = rows_of(gather_tp([(n * gain_mlp).astype(BF16) for n in normed_two], size))

    dm = rows_of(gather_tp([after(g.astype(BF16), h1_slot[-1]) for g in grad_rows], size, h2))

    hid, gate_slope, up_slope = gate_up(h2, gate_full, up_full)
    down_term = matmul_tn(dm, hid).astype(BF16)
    grad_gate, grad_up = hidden_back(dm, down_full, after(gate_slope, down_term), up_slope)
    half_group, quarter = group // 2, group // 4
    two = {}
    two[2] = two_nt(grad_gate, grad_up, gate_full, up_full, half_group, half_group)
    two[1] = two_nt(after(grad_gate, two[2]), grad_up, gate_full, up_full, quarter, quarter)
    two[0] = two_nt(after(grad_gate, two[1]), grad_up, gate_full, up_full, 0, quarter)
    gate_term = matmul_tn(h2, after(grad_gate, two[0])).astype(BF16)
    up_term = matmul_tn(h2, after(grad_up, gate_term)).astype(BF16)
    mlp = matmul_nt(after(hid, up_term), down_full).astype(BF16)

    def two_piece(r):
        i = (r >= size // 4) + (r >= size // 2)
        inside = r - (0, size // 4, size // 2)[i]
        return two[i][inside * own : (inside + 1) * own]

    grad_two = scatter_tp(two_piece, size)
    gain_mlp_term = sum(jnp.sum(g * n, axis=0) for g, n in zip(grad_two, normed_two))
    inner_two = [g * gain_mlp for g in grad_two]
    grad_middle = [
        g + s * (i - n * jnp.mean(i * n, axis=-1, keepdims=True))
        for g, s, i, n in zip(grad_rows, scale_two, inner_two, normed_two)
    ]
    grad_attn = rows_of(gather_tp([after(g.astype(BF16), gate_term) for g in grad_middle], size))
    down_grad = back_fsdp(down_term)
    gate_grad = back_fsdp(gate_term)
    up_grad = back_fsdp(up_term)
    mlp, grad_attn, down_grad = lax.optimization_barrier((mlp, grad_attn, down_grad))
    mlp_out = scatter_tp(lambda r: mlp[r * own : (r + 1) * own], size, settle=True)
    output = jnp.concatenate(
        [(m * (v + o)).astype(BF16) for m, v, o in zip(valid, middle, mlp_out)], axis=0
    )

    grad_mixed = matmul(grad_attn, out_full).astype(BF16)
    grad_qkv = {}
    partial_one = {}
    last = None
    for s in reversed(range(count)):
        query, keys, values, mixed_s, log_total = saved[s]
        if last is not None:
            query = after(query, last)
        grad_qkv[s] = attend_back(query, keys, values, mixed_s, log_total, grad_mixed, s, infos[s], cosine, sine, own, length)
        if s:
            last = partial_one[s] = matmul_nt(grad_qkv[s], qkv_full).astype(BF16)
        if s == count - 1:
            mixed = after(jnp.concatenate([saved[i][3] for i in range(count)], axis=0), last)
            last = out_term = matmul_tn(grad_attn, mixed).astype(BF16)
    grad_all = jnp.concatenate([grad_qkv[s] for s in range(count)], axis=0)
    qkv_term = matmul_tn(rows_of(h1_slot), grad_all).astype(BF16)
    partial_one[0] = matmul_nt(after(grad_qkv[0], qkv_term, gate_grad, up_grad), qkv_full).astype(BF16)

    def one_piece(r):
        s, inside = divmod(r, per_slot)
        return partial_one[s][inside * own : (inside + 1) * own]

    grad_one = scatter_tp(one_piece, size)
    qkv_held = after(qkv_term, partial_one[0]).astype(F32)
    gain_attn_term = jnp.sum(qkv_held * qkv_full.astype(F32), axis=1) / gain_attn
    inner_one = [g * gain_attn for g in grad_one]
    input_grad = jnp.concatenate(
        [
            (m + s * (i - n * jnp.mean(i * n, axis=-1, keepdims=True))).astype(BF16)
            for m, s, i, n in zip(grad_middle, scale_one, inner_one, normed_one)
        ],
        axis=0,
    )

    out_proj_grad = back_fsdp(out_term)
    qkv_grad = back_fsdp(qkv_term)
    gains = scatter_vectors(jnp.stack([gain_attn_term, gain_mlp_term]))
    return (
        output,
        input_grad,
        gains[0],
        gains[1],
        qkv_grad[:, :head_width],
        qkv_grad[:, head_width : 2 * head_width],
        qkv_grad[:, 2 * head_width :],
        out_proj_grad,
        gate_grad,
        up_grad,
        down_grad,
    )


def solution(mesh):
    rows = P(("fsdp", "tp"), None)
    weight = P("fsdp", "tp")
    vector = P(("fsdp", "tp"))
    return jax.shard_map(
        per_device,
        mesh=mesh,
        in_specs=(rows, P(), P()) + (weight,) * 7 + (P("fsdp"), rows),
        out_specs=(rows, rows, vector, vector) + (weight,) * 7,
        check_vma=False,
    )
```
